256 devices in a mesh: dp: 8 (over x, core), expert: 32 (over z, y).
Axes of the slice: x: 4, y: 4, z: 8, core: 2. Of those that a mesh axis runs over, the one named last changes fastest.
Arguments:
- tokens: bfloat16 [5120, 262144], P(None, ('dp', 'expert')), may hold values from -24 to 24, as said below
- router: bfloat16 [5120, 160], P(None, 'expert'), may hold values from -1 to 1, as said below
- device_pick: int32 [3, 262144], P(None, 'dp'), may hold values from 0 to 31, as said below
- expert_pick: int32 [6, 262144], P(None, 'dp'), may hold values from 0 to 159, as said below
Outputs:
- gates: float32 [6, 262144], P(None, 'dp')
- device_max: float32 [32, 262144], P('expert', 'dp')
- balance: float32 [3], replicated
The draws below stay inside these ranges and needn't reach their ends.
Inputs may be any that keep to these rules, and one draw needn't show every extreme that they name: tokens lie within the range; in each column the values are of order one, except in a few columns. router entries are of order 1 / sqrt(5120). `device_pick`: each column names 3 different devices. `expert_pick`: each column names 6 different experts, two on each device of the column's device_pick, in that order; the device of expert e is e // 5.
All inputs are finite; a program needn't handle non-finite values.
Results may differ from the reference program's by a relative error of at most 0.0003.
Values may be sent and summed in bfloat16 or wider, within the bound.
No kernel may reach another device: no remote copies, remote signals or barrier semaphores. Data moves between devices by JAX's collectives and lax.ppermute only.
A program may use at most 64 MiB of HBM per device.

```python
import jax
import jax.numpy as jnp
from jax import lax

D = 5120
EXP_DEV = 5
TOP = 6
DEV_TOP = 3
TOK_DEV = 32768
NDEV = 32
E = 160
TOKENS = 262144


def router_base(key):
    values = jax.random.normal(jax.random.fold_in(key, 7), (D, E), jnp.float32)
    return jnp.clip(values, -6.0, 6.0) * D ** (-0.5)


def draw_router(key, part):
    return router_base(key).astype(jnp.bfloat16)


def draw_tokens(key, part):
    inner = jax.random.fold_in(key, 3)
    shared = jax.random.normal(jax.random.fold_in(inner, 1), (D,), jnp.float32) * 0.5
    values = jax.random.normal(jax.random.fold_in(inner, 4), (TOKENS, D), jnp.float32) + shared[None, :]
    return jnp.clip(values, -24.0, 24.0).T.astype(jnp.bfloat16)


def draw_picks(key):
    inner = jax.random.fold_in(key, 11)
    span = max(TOK_DEV // 2, 1)
    blocks = (TOKENS + span - 1) // span
    hot_table = jax.random.randint(jax.random.fold_in(inner, 1), (blocks, 4), 0, NDEV)
    rows = jnp.arange(TOKENS, dtype=jnp.int32)
    hot_rows = hot_table[rows // span]
    slots = jnp.arange(NDEV, dtype=jnp.int32)
    hot = jnp.any(hot_rows[:, :, None] == slots[None, None, :], axis=1).astype(jnp.int32)
    noise = jax.random.randint(jax.random.fold_in(inner, 2), (TOKENS, NDEV), 0, 2 ** 22)
    keyed = (noise + hot * 2 ** 21) * NDEV + slots[None, :]
    _, chosen_dev = lax.top_k(keyed, DEV_TOP)
    chosen_dev = chosen_dev.astype(jnp.int32)
    local_noise = jax.random.randint(jax.random.fold_in(inner, 3), (TOKENS, DEV_TOP, EXP_DEV), 0, 2 ** 20)
    local_keyed = local_noise * EXP_DEV + jnp.arange(EXP_DEV, dtype=jnp.int32)[None, None, :]
    _, local_slot = lax.top_k(local_keyed, 2)
    experts = chosen_dev[:, :, None] * EXP_DEV + local_slot.astype(jnp.int32)
    return (chosen_dev.T, experts.reshape(TOKENS, TOP).T.astype(jnp.int32))


def draw_device_pick(key, part):
    return draw_picks(key)[0]


def draw_expert_pick(key, part):
    return draw_picks(key)[1]


def setup_inputs(seed: int = 0) -> dict:
    keys = jax.random.split(jax.random.key(seed), 5)
    tokens = draw_tokens(jax.random.fold_in(keys[4], 71), 0)
    router = draw_router(jax.random.fold_in(keys[4], 71), 0)
    device_pick = draw_device_pick(jax.random.fold_in(keys[4], 71), 0)
    expert_pick = draw_expert_pick(jax.random.fold_in(keys[4], 71), 0)
    return {"tokens": tokens, "router": router, "device_pick": device_pick, "expert_pick": expert_pick}


def reference(tokens, router, device_pick, expert_pick):
    scores = jnp.dot(router.T, tokens, preferred_element_type=jnp.float32)
    peak = jnp.max(scores, axis=0, keepdims=True)
    raised = jnp.exp(scores - peak)
    probs = raised / jnp.sum(raised, axis=0, keepdims=True)
    gates = jnp.take_along_axis(probs, expert_pick, axis=0)
    device_max = jnp.max(probs.reshape(NDEV, EXP_DEV, TOKENS), axis=1)
    ones_exp = jnp.ones((TOKENS * TOP,), jnp.float32)
    counts = jax.ops.segment_sum(ones_exp, expert_pick.reshape(-1), num_segments=E)
    ones_dev = jnp.ones((TOKENS * DEV_TOP,), jnp.float32)
    sent_counts = jax.ops.segment_sum(ones_dev, device_pick.reshape(-1), num_segments=NDEV)
    freq = counts * (E / (TOP * TOKENS))
    prob = jnp.sum(probs, axis=1) / TOKENS
    dev_freq = jnp.mean(freq.reshape(NDEV, EXP_DEV), axis=1)
    dev_prob = jnp.sum(prob.reshape(NDEV, EXP_DEV), axis=1)
    sent = sent_counts * (NDEV / (DEV_TOP * TOKENS))
    balance = jnp.stack([jnp.sum(freq * prob), jnp.sum(dev_freq * dev_prob), jnp.sum(sent * dev_prob)])
    return gates, device_max, balance
```

```python
import functools

import jax
import jax.numpy as jnp
from jax import lax
from jax.experimental import pallas as pl
from jax.experimental.pallas import tpu as pltpu
from jax.sharding import Mesh
from jax.sharding import PartitionSpec as P

TOP = 6
DEV_TOP = 3
EXPERT = ("expert_0", "expert_1")
DP = ("dp_0", "dp_1")
DP_EXPERT = ("dp_0", "dp_1", "expert_0", "expert_1")
BLOCK = 256
LANES = 128


def sent_to_all(x, axis):
    length = lax.axis_size(axis)
    return lax.all_to_all(jnp.broadcast_to(x[None], (length, *x.shape)), axis, 0, 0, tiled=True)


def lane_sum(x):
    parts = [x[:, i : i + LANES] for i in range(0, x.shape[1], LANES)]
    return functools.reduce(jnp.add, parts)


def route_kernel(num_devices, per_device, where, router, tokens, picks, devs, out, prob_acc, count_acc, sent_acc):
    step = pl.program_id(0)
    num_experts = num_devices * per_device
    block = tokens.shape[1]

    @pl.when(step == 0)
    def _():
        prob_acc[...] = jnp.zeros_like(prob_acc)
        count_acc[...] = jnp.zeros_like(count_acc)
        sent_acc[...] = jnp.zeros_like(sent_acc)

    scores = jnp.dot(router[...], tokens[...], preferred_element_type=jnp.float32)
    peak = jnp.max(scores, axis=0, keepdims=True)
    raised = jnp.exp(scores - peak)
    probs = raised / jnp.sum(raised, axis=0, keepdims=True)
    prob_acc[...] += lane_sum(probs)
    rows = lax.broadcasted_iota(jnp.int32, (num_experts, block), 0)
    ids = (rows % num_devices) * per_device + rows // num_devices
    chosen = []
    hits = jnp.zeros((num_experts, block), jnp.float32)
    for k in range(TOP):
        mask = ids == picks[k : k + 1, :]
        chosen.append(jnp.sum(jnp.where(mask, probs, 0.0), axis=0, keepdims=True))
        hits += jnp.where(mask, 1.0, 0.0)
    count_acc[...] += lane_sum(hits)
    dev_ids = lax.broadcasted_iota(jnp.int32, (num_devices, block), 0)
    sent = jnp.zeros((num_devices, block), jnp.float32)
    for k in range(DEV_TOP):
        sent += jnp.where(dev_ids == devs[k : k + 1, :], 1.0, 0.0)
    sent_acc[...] += lane_sum(sent)
    gates = jnp.concatenate(chosen, axis=0)
    maxima = functools.reduce(
        jnp.maximum, [probs[j * num_devices : (j + 1) * num_devices] for j in range(per_device)]
    )
    cols = pl.ds(step * block, block)
    for d in range(num_devices):
        out[d, 0:TOP, cols] = gates
        out[d, TOP : TOP + 1, cols] = maxima[d : d + 1]

    @pl.when(step == pl.num_programs(0) - 1)
    def _():
        def row(acc, width):
            line = jnp.sum(acc[...].T, axis=0, keepdims=True)
            return jnp.concatenate([line, jnp.zeros((1, width - line.shape[1]), jnp.float32)], axis=1)

        sums = jnp.concatenate(
            [row(prob_acc, 256), row(count_acc, 256), row(sent_acc, 512)], axis=1
        )
        for d in range(num_devices):
            out[d, TOP + 1 : TOP + 2, :] = sums


def spread_kernel(recv, gates, maxima, sums):
    num, _, share = recv.shape
    total = jnp.zeros((1, share), jnp.float32)
    for d in range(num):
        cols = slice(d * share, (d + 1) * share)
        gates[:, cols] = recv[d, 0:TOP, :]
        maxima[:, cols] = recv[d, TOP : TOP + 1, :]
        total += recv[d, TOP + 1 : TOP + 2, :]
    sums[...] = jnp.broadcast_to(total, sums.shape)


def local(tokens, router, device_pick, expert_pick):
    features, share = tokens.shape
    num_devices = lax.axis_size(EXPERT)
    per_device = router.shape[1]
    num_experts = per_device * num_devices
    total_tokens = share * num_devices * lax.axis_size(DP)
    my_index = lax.axis_index(EXPERT)
    core = lax.axis_index("dp_1")
    half = features // 2

    mine = lax.dynamic_slice_in_dim(router.T, core * half, half, 1)
    packed = sent_to_all(mine.reshape(per_device * half // LANES, LANES), EXPERT)
    ours = packed.reshape(num_devices, per_device, half).transpose(1, 0, 2).reshape(num_experts, half)
    theirs = lax.ppermute(ours, "dp_1", [(0, 1), (1, 0)])
    first = jnp.where(core == 0, ours, theirs)
    second = jnp.where(core == 0, theirs, ours)
    full = jnp.concatenate([first, second], axis=1)

    steps = share // BLOCK
    where = my_index.astype(jnp.int32).reshape(1)
    msg = pl.pallas_call(
        functools.partial(route_kernel, num_devices, per_device),
        out_shape=jax.ShapeDtypeStruct((num_devices, TOP + 2, share), jnp.float32),
        grid_spec=pltpu.PrefetchScalarGridSpec(
            num_scalar_prefetch=1,
            grid=(steps,),
            in_specs=[
                pl.BlockSpec((num_experts, features), lambda i, w: (0, 0)),
                pl.BlockSpec((features, BLOCK), lambda i, w: (0, i)),
                pl.BlockSpec((TOP, BLOCK), lambda i, w: (0, w[0] * steps + i)),
                pl.BlockSpec((DEV_TOP, BLOCK), lambda i, w: (0, w[0] * steps + i)),
            ],
            out_specs=pl.BlockSpec((num_devices, TOP + 2, share), lambda i, w: (0, 0, 0)),
            scratch_shapes=[
                pltpu.VMEM((num_experts, LANES), jnp.float32),
                pltpu.VMEM((num_experts, LANES), jnp.float32),
                pltpu.VMEM((num_devices, LANES), jnp.float32),
            ],
        ),
        compiler_params=pltpu.CompilerParams(
            dimension_semantics=("arbitrary",), vmem_limit_bytes=32 * 1024 * 1024
        ),
        name="route",
    )(where, full, tokens, expert_pick, device_pick)

    recv = lax.all_to_all(msg, EXPERT, 0, 0, tiled=True)
    gates, device_max, sums = pl.pallas_call(
        spread_kernel,
        out_shape=(
            jax.ShapeDtypeStruct((TOP, share * num_devices), jnp.float32),
            jax.ShapeDtypeStruct((1, share * num_devices), jnp.float32),
            jax.ShapeDtypeStruct((8, share), jnp.float32),
        ),
        compiler_params=pltpu.CompilerParams(vmem_limit_bytes=16 * 1024 * 1024),
        name="spread",
    )(recv)
    sums = jnp.sum(sent_to_all(sums[0:1, 0:768].reshape(6, LANES), DP), axis=0).reshape(768)
    prob_sum = sums[0:num_experts]
    counts = sums[256 : 256 + num_experts]
    sent_counts = sums[512 : 512 + num_devices]
    freq = counts * (num_experts / (TOP * total_tokens))
    prob = prob_sum / total_tokens
    dev_freq = jnp.mean(freq.reshape(per_device, num_devices), axis=0)
    dev_prob = jnp.sum(prob.reshape(per_device, num_devices), axis=0)
    sent = sent_counts * (num_devices / (DEV_TOP * total_tokens))
    balance = jnp.stack(
        [jnp.sum(freq * prob), jnp.sum(dev_freq * dev_prob), jnp.sum(sent * dev_prob)]
    )
    return (gates, device_max, balance)


def solution(mesh):
    torus = Mesh(mesh.devices.reshape(4, 2, 8, 4), ("dp_0", "dp_1", "expert_0", "expert_1"))
    return jax.shard_map(
        local,
        mesh=torus,
        in_specs=(P(None, DP_EXPERT), P(None, EXPERT), P(None, DP), P(None, DP)),
        out_specs=(P(None, DP), P(EXPERT, DP), P()),
        check_vma=False,
    )
```

```python
import functools

import jax
import jax.numpy as jnp
from jax import lax
from jax.experimental import pallas as pl
from jax.experimental.pallas import tpu as pltpu
from jax.sharding import Mesh
from jax.sharding import PartitionSpec as P

TOP = 6
DEV_TOP = 3
EXPERT = ("expert_0", "expert_1")
DP = ("dp_0", "dp_1")
DP_EXPERT = ("dp_0", "dp_1", "expert_0", "expert_1")
BLOCK = 256
LANES = 128
ROWS = 8
TOP_CODE = 65535.0
MIDDLE = 32768
TINY = 1e-30


def sent_to_all(x, axis):
    length = lax.axis_size(axis)
    return lax.all_to_all(jnp.broadcast_to(x[None], (length, *x.shape)), axis, 0, 0, tiled=True)


def lane_sum(x):
    parts = [x[:, i : i + LANES] for i in range(0, x.shape[1], LANES)]
    return functools.reduce(jnp.add, parts)


def fourth(x):
    return jnp.square(jnp.square(x))


def eighth(x):
    return jnp.square(fourth(x))


def eighth_root(x):
    return jnp.sqrt(jnp.sqrt(jnp.sqrt(x)))


def unit(code):
    return code * (1.0 / TOP_CODE)


def step_scale(code):
    return jnp.maximum(eighth(unit(code)), TINY) * (1.0 / TOP_CODE)


def coded_pair(x, limit):
    coarse = jnp.minimum(jnp.floor(eighth_root(x * (1.0 / limit)) * TOP_CODE), TOP_CODE)
    base = eighth(unit(coarse)) * limit
    rest = jnp.where(base > 0.0, (x - base) / jnp.maximum(base, TINY), 0.0)
    fine = jnp.round(jnp.clip(rest * coarse * (1.0 / 16.0), 0.0, 1.0) * TOP_CODE)
    return coarse, fine


def decoded_pair(coarse, fine, limit):
    base = eighth(unit(coarse)) * limit
    return base * (1.0 + unit(fine) * 16.0 / jnp.maximum(coarse, 1.0))


def route_kernel(num_devices, per_device, where, router, tokens, picks, devs, out, prob_acc, count_acc, sent_acc):
    step = pl.program_id(0)
    num_experts = num_devices * per_device
    block = tokens.shape[1]
    tiles = block // LANES
    share = block * pl.num_programs(0)

    @pl.when(step == 0)
    def _():
        prob_acc[...] = jnp.zeros_like(prob_acc)
        count_acc[...] = jnp.zeros_like(count_acc)
        sent_acc[...] = jnp.zeros_like(sent_acc)

    scores = jnp.dot(router[...], tokens[...], preferred_element_type=jnp.float32)
    peak = jnp.max(scores, axis=0, keepdims=True)
    raised = jnp.exp(scores - peak)
    probs = raised / jnp.sum(raised, axis=0, keepdims=True)
    prob_acc[...] += lane_sum(probs)
    rows = lax.broadcasted_iota(jnp.int32, (num_experts, block), 0)
    ids = (rows % num_devices) * per_device + rows // num_devices
    chosen = []
    hits = jnp.zeros((num_experts, block), jnp.float32)
    for k in range(TOP):
        mask = ids == picks[k : k + 1, :]
        chosen.append(jnp.sum(jnp.where(mask, probs, 0.0), axis=0, keepdims=True))
        hits += jnp.where(mask, 1.0, 0.0)
    count_acc[...] += lane_sum(hits)
    dev_ids = lax.broadcasted_iota(jnp.int32, (num_devices, block), 0)
    sent = jnp.zeros((num_devices, block), jnp.float32)
    for k in range(DEV_TOP):
        sent += jnp.where(dev_ids == devs[k : k + 1, :], 1.0, 0.0)
    sent_acc[...] += lane_sum(sent)

    largest = functools.reduce(jnp.maximum, chosen)
    scale = jnp.minimum(jnp.floor(eighth_root(largest) * TOP_CODE) + 1.0, TOP_CODE)
    inverse = 1.0 / step_scale(scale)
    codes = [jnp.minimum(jnp.round(g * inverse), TOP_CODE) for g in chosen]
    lines = jnp.concatenate([*codes, scale, scale], axis=0).astype(jnp.int32) - MIDDLE
    maxima = functools.reduce(
        jnp.maximum, [probs[j * num_devices : (j + 1) * num_devices] for j in range(per_device)]
    )
    max_codes = jnp.round(jnp.sqrt(jnp.sqrt(maxima)) * TOP_CODE).astype(jnp.int32) - MIDDLE
    max_codes = jnp.minimum(max_codes, MIDDLE - 1)
    stacked = jnp.concatenate([lines[:, j * LANES : (j + 1) * LANES] for j in range(tiles)], axis=0)
    last = lax.broadcasted_iota(jnp.int32, stacked.shape, 0) % ROWS == ROWS - 1
    here = pl.ds(pl.multiple_of(step * tiles * ROWS, tiles * ROWS), tiles * ROWS)
    for d in range(num_devices):
        line = jnp.concatenate(
            [
                jnp.broadcast_to(max_codes[d : d + 1, j * LANES : (j + 1) * LANES], (ROWS, LANES))
                for j in range(tiles)
            ],
            axis=0,
        )
        out[d, here, :] = jnp.where(last, line, stacked).astype(jnp.int16)

    @pl.when(step == pl.num_programs(0) - 1)
    def _():
        def row(acc):
            line = jnp.sum(acc[...].T, axis=0, keepdims=True)
            missing = 2 * LANES - line.shape[1]
            line = jnp.concatenate([line, jnp.zeros((1, missing), jnp.float32)], axis=1)
            return line[:, :LANES], line[:, LANES:]

        low, high = row(prob_acc)
        low_coarse, low_fine = coded_pair(low, share)
        high_coarse, high_fine = coded_pair(high, share)
        count_low, count_high = row(count_acc)
        sent_low, sent_high = row(sent_acc)
        sums = jnp.concatenate(
            [low_coarse, high_coarse, low_fine, high_fine, count_low, count_high, sent_low, sent_high], axis=0
        )
        sums = (sums.astype(jnp.int32) - MIDDLE).astype(jnp.int16)
        for d in range(num_devices):
            out[d, pl.ds(share // LANES * ROWS, ROWS), :] = sums


def spread_kernel(recv, gates, maxima, sums):
    num, rows, _ = recv.shape
    tiles = rows // ROWS - 1
    share = tiles * LANES
    total = jnp.zeros((ROWS, LANES), jnp.float32)
    for d in range(num):
        codes = recv[d].astype(jnp.int32).astype(jnp.float32) + float(MIDDLE)
        for j in range(tiles):
            tile = codes[j * ROWS : (j + 1) * ROWS]
            cols = slice(d * share + j * LANES, d * share + (j + 1) * LANES)
            gates[:, cols] = tile[0:TOP] * step_scale(tile[TOP : TOP + 1])
            maxima[:, cols] = fourth(unit(tile[TOP + 1 : TOP + 2]))
        tile = codes[tiles * ROWS :]
        probs = decoded_pair(tile[0:2], tile[2:4], share)
        total += jnp.concatenate([probs, tile[4:8], jnp.zeros((2, LANES), jnp.float32)], axis=0)
    sums[...] = total


def balance_kernel(num_devices, per_device, total_tokens, where, own, first, second, third, out, slots):
    place = where[0]
    for k, part in enumerate((own, first, second, third)):
        slots[(place + 4 - k) % 4] = part[...]
    total = (slots[0] + slots[1]) + (slots[2] + slots[3])
    num_experts = num_devices * per_device
    prob = jnp.concatenate([total[0:1], total[1:2]], axis=1)[:, :num_experts] / total_tokens
    freq = jnp.concatenate([total[2:3], total[3:4]], axis=1)[:, :num_experts] * (
        num_experts / (TOP * total_tokens)
    )
    sent = total[4:5, :num_devices] * (num_devices / (DEV_TOP * total_tokens))

    def by_device(x):
        return functools.reduce(
            jnp.add, [x[:, j * num_devices : (j + 1) * num_devices] for j in range(per_device)]
        )

    dev_prob = by_device(prob)
    dev_freq = by_device(freq) / per_device
    losses = [jnp.sum(a * b, axis=1, keepdims=True) for a, b in ((freq, prob), (dev_freq, dev_prob), (sent, dev_prob))]
    lane = lax.broadcasted_iota(jnp.int32, (1, LANES), 1)
    out[...] = jnp.where(lane == 0, losses[0], jnp.where(lane == 1, losses[1], losses[2]))


def local(tokens, router, device_pick, expert_pick):
    features, share = tokens.shape
    num_devices = lax.axis_size(EXPERT)
    per_device = router.shape[1]
    num_experts = per_device * num_devices
    total_tokens = share * num_devices * lax.axis_size(DP)
    my_index = lax.axis_index(EXPERT)
    core = lax.axis_index("dp_1")
    half = features // 2

    mine = lax.dynamic_slice_in_dim(router.T, core * half, half, 1)
    packed = sent_to_all(mine.reshape(per_device * half // LANES, LANES), EXPERT)
    ours = packed.reshape(num_devices, per_device, half).transpose(1, 0, 2).reshape(num_experts, half)
    theirs = lax.ppermute(ours, "dp_1", [(0, 1), (1, 0)])
    first = jnp.where(core == 0, ours, theirs)
    second = jnp.where(core == 0, theirs, ours)
    full = jnp.concatenate([first, second], axis=1)

    steps = share // BLOCK
    where = my_index.astype(jnp.int32).reshape(1)
    rows = (share // LANES + 1) * ROWS
    msg = pl.pallas_call(
        functools.partial(route_kernel, num_devices, per_device),
        out_shape=jax.ShapeDtypeStruct((num_devices, rows, LANES), jnp.int16),
        grid_spec=pltpu.PrefetchScalarGridSpec(
            num_scalar_prefetch=1,
            grid=(steps,),
            in_specs=[
                pl.BlockSpec((num_experts, features), lambda i, w: (0, 0)),
                pl.BlockSpec((features, BLOCK), lambda i, w: (0, i)),
                pl.BlockSpec((TOP, BLOCK), lambda i, w: (0, w[0] * steps + i)),
                pl.BlockSpec((DEV_TOP, BLOCK), lambda i, w: (0, w[0] * steps + i)),
            ],
            out_specs=pl.BlockSpec((num_devices, rows, LANES), lambda i, w: (0, 0, 0)),
            scratch_shapes=[
                pltpu.VMEM((num_experts, LANES), jnp.float32),
                pltpu.VMEM((num_experts, LANES), jnp.float32),
                pltpu.VMEM((num_devices, LANES), jnp.float32),
            ],
        ),
        compiler_params=pltpu.CompilerParams(
            dimension_semantics=("arbitrary",), vmem_limit_bytes=52 * 1024 * 1024
        ),
        name="route",
    )(where, full, tokens, expert_pick, device_pick)

    recv = lax.all_to_all(msg, EXPERT, 0, 0, tiled=True)
    gates, device_max, sums = pl.pallas_call(
        spread_kernel,
        out_shape=(
            jax.ShapeDtypeStruct((TOP, share * num_devices), jnp.float32),
            jax.ShapeDtypeStruct((1, share * num_devices), jnp.float32),
            jax.ShapeDtypeStruct((ROWS, LANES), jnp.float32),
        ),
        compiler_params=pltpu.CompilerParams(vmem_limit_bytes=16 * 1024 * 1024),
        name="spread",
    )(recv)
    chip = sums + lax.ppermute(sums, "dp_1", [(0, 1), (1, 0)])
    length = lax.axis_size("dp_0")
    others = [
        lax.ppermute(chip, "dp_0", [(i, (i + k) % length) for i in range(length)]) for k in range(1, length)
    ]
    balance = pl.pallas_call(
        functools.partial(balance_kernel, num_devices, per_device, total_tokens),
        out_shape=jax.ShapeDtypeStruct((1, LANES), jnp.float32),
        grid_spec=pltpu.PrefetchScalarGridSpec(
            num_scalar_prefetch=1,
            grid=(1,),
            in_specs=[pl.BlockSpec((ROWS, LANES), lambda i, w: (0, 0))] * 4,
            out_specs=pl.BlockSpec((1, LANES), lambda i, w: (0, 0)),
            scratch_shapes=[pltpu.VMEM((4, ROWS, LANES), jnp.float32)],
        ),
        compiler_params=pltpu.CompilerParams(vmem_limit_bytes=1024 * 1024),
        name="balance",
    )(lax.axis_index("dp_0").astype(jnp.int32).reshape(1), chip, *others)
    return (gates, device_max, balance[0, 0:3])


def solution(mesh):
    torus = Mesh(mesh.devices.reshape(4, 2, 8, 4), ("dp_0", "dp_1", "expert_0", "expert_1"))
    return jax.shard_map(
        local,
        mesh=torus,
        in_specs=(P(None, DP_EXPERT), P(None, EXPERT), P(None, DP), P(None, DP)),
        out_specs=(P(None, DP), P(EXPERT, DP), P()),
        check_vma=False,
    )
```

```python
import functools

import jax
import jax.numpy as jnp
from jax import lax
from jax.experimental import pallas as pl
from jax.experimental.pallas import tpu as pltpu
from jax.sharding import Mesh
from jax.sharding import PartitionSpec as P

TOP = 6
DEV_TOP = 3
EXPERT = ("expert_0", "expert_1")
DP = ("dp_0", "dp_1")
DP_EXPERT = ("dp_0", "dp_1", "expert_0", "expert_1")
BLOCK = 256
LANES = 128
ROWS = 8
TOP_CODE = 65535.0
MIDDLE = 32768
TINY = 1e-30


def sent_to_all(x, axis):
    length = lax.axis_size(axis)
    return lax.all_to_all(jnp.broadcast_to(x[None], (length, *x.shape)), axis, 0, 0, tiled=True)


def lane_sum(x):
    parts = [x[:, i : i + LANES] for i in range(0, x.shape[1], LANES)]
    return functools.reduce(jnp.add, parts)


def fourth(x):
    return jnp.square(jnp.square(x))


def eighth(x):
    return jnp.square(fourth(x))


def eighth_root(x):
    return jnp.sqrt(jnp.sqrt(jnp.sqrt(x)))


def unit(code):
    return code * (1.0 / TOP_CODE)


def step_scale(code):
    return jnp.maximum(eighth(unit(code)), TINY) * (1.0 / TOP_CODE)


def coded_pair(x, limit):
    coarse = jnp.minimum(jnp.floor(eighth_root(x * (1.0 / limit)) * TOP_CODE), TOP_CODE)
    base = eighth(unit(coarse)) * limit
    rest = jnp.where(base > 0.0, (x - base) / jnp.maximum(base, TINY), 0.0)
    fine = jnp.round(jnp.clip(rest * coarse * (1.0 / 16.0), 0.0, 1.0) * TOP_CODE)
    return coarse, fine


def decoded_pair(coarse, fine, limit):
    base = eighth(unit(coarse)) * limit
    return base * (1.0 + unit(fine) * 16.0 / jnp.maximum(coarse, 1.0))


def source_device(core, place, row, half, sizes):
    deep, wide = sizes
    z, y = place
    back = row % (deep // 2)
    aside = (row // (deep // 2)) % wide
    ahead = jnp.where(back == 0, deep // 2, back)
    offset = jnp.where(core == half, deep - back, ahead)
    return ((z + offset) % deep) * wide + (y + wide - aside) % wide


def route_kernel(
    sizes, per_device, where, own, other, tokens, picks, devs, out, router, prob_acc, count_acc, sent_acc
):
    step = pl.program_id(0)
    deep, wide = sizes
    num_devices = deep * wide
    num_experts = num_devices * per_device
    group = num_devices // 2
    rows_half = num_experts // 2
    block = tokens.shape[1]
    tiles = block // LANES
    share = block * pl.num_programs(0)
    core, place = where[1], (where[2], where[3])

    @pl.when(step == 0)
    def _():
        router[:rows_half] = own[...]
        router[rows_half:] = other[...]
        prob_acc[...] = jnp.zeros_like(prob_acc)
        count_acc[...] = jnp.zeros_like(count_acc)
        sent_acc[...] = jnp.zeros_like(sent_acc)

    row = lax.broadcasted_iota(jnp.int32, (num_experts, LANES), 0)
    half = row // rows_half
    dev = source_device(core, place, row % group, half, sizes)
    slot = (row % rows_half) // group
    ids = dev * per_device + slot
    ids_wide = jnp.concatenate([ids] * tiles, axis=1)

    scores = jnp.dot(router[...], tokens[...], preferred_element_type=jnp.float32)
    peak = jnp.max(scores, axis=0, keepdims=True)
    raised = jnp.exp(scores - peak)
    probs = raised / jnp.sum(raised, axis=0, keepdims=True)
    prob_acc[...] += lane_sum(probs)
    chosen = []
    hits = jnp.zeros((num_experts, block), jnp.float32)
    for k in range(TOP):
        mask = ids_wide == picks[k : k + 1, :]
        chosen.append(jnp.sum(jnp.where(mask, probs, 0.0), axis=0, keepdims=True))
        hits += jnp.where(mask, 1.0, 0.0)
    count_acc[...] += lane_sum(hits)
    dev_ids = lax.broadcasted_iota(jnp.int32, (num_devices, block), 0)
    sent = jnp.zeros((num_devices, block), jnp.float32)
    for k in range(DEV_TOP):
        sent += jnp.where(dev_ids == devs[k : k + 1, :], 1.0, 0.0)
    sent_acc[...] += lane_sum(sent)

    largest = functools.reduce(jnp.maximum, chosen)
    scale = jnp.minimum(jnp.floor(eighth_root(largest) * TOP_CODE) + 1.0, TOP_CODE)
    inverse = 1.0 / step_scale(scale)
    codes = [jnp.minimum(jnp.round(g * inverse), TOP_CODE) for g in chosen]
    lines = jnp.concatenate([*codes, scale, scale], axis=0).astype(jnp.int32) - MIDDLE
    stacked = jnp.concatenate([lines[:, j * LANES : (j + 1) * LANES] for j in range(tiles)], axis=0)
    last = lax.broadcasted_iota(jnp.int32, stacked.shape, 0) % ROWS == ROWS - 1
    here = pl.ds(pl.multiple_of(step * tiles * ROWS, tiles * ROWS), tiles * ROWS)
    for h in range(2):
        slabs = [probs[h * rows_half + j * group : h * rows_half + (j + 1) * group] for j in range(per_device)]
        maxima = functools.reduce(jnp.maximum, slabs)
        max_codes = jnp.round(jnp.sqrt(jnp.sqrt(maxima)) * TOP_CODE).astype(jnp.int32) - MIDDLE
        max_codes = jnp.minimum(max_codes, MIDDLE - 1)
        for s in range(group):
            line = jnp.concatenate(
                [
                    jnp.broadcast_to(max_codes[s : s + 1, j * LANES : (j + 1) * LANES], (ROWS, LANES))
                    for j in range(tiles)
                ],
                axis=0,
            )
            target = source_device(core, place, s, h, sizes)
            out[target, here, :] = jnp.where(last, line, stacked).astype(jnp.int16)

    @pl.when(step == pl.num_programs(0) - 1)
    def _():
        def lined(acc, index):
            total = jnp.sum(acc[...], axis=1, keepdims=True)
            lanes = lax.broadcasted_iota(jnp.int32, index.shape, 1)
            parts = [
                jnp.sum(jnp.where(index == lanes + i * LANES, total, 0.0), axis=0, keepdims=True) for i in range(2)
            ]
            return parts

        order = slot * num_devices + dev
        low, high = lined(prob_acc, order)
        low_coarse, low_fine = coded_pair(low, share)
        high_coarse, high_fine = coded_pair(high, share)
        count_low, count_high = lined(count_acc, order)
        sent_low, sent_high = lined(sent_acc, lax.broadcasted_iota(jnp.int32, (num_devices, LANES), 0))
        sums = jnp.concatenate(
            [low_coarse, high_coarse, low_fine, high_fine, count_low, count_high, sent_low, sent_high], axis=0
        )
        sums = (sums.astype(jnp.int32) - MIDDLE).astype(jnp.int16)
        for d in range(num_devices):
            out[d, pl.ds(share // LANES * ROWS, ROWS), :] = sums


def decoded(codes):
    return codes.astype(jnp.int32).astype(jnp.float32) + float(MIDDLE)


def sums_kernel(share, recv, sums):
    total = jnp.zeros((ROWS, LANES), jnp.float32)
    for d in range(recv.shape[0]):
        tile = decoded(recv[d])
        probs = decoded_pair(tile[0:2], tile[2:4], share)
        total += jnp.concatenate([probs, tile[4:8], jnp.zeros((2, LANES), jnp.float32)], axis=0)
    sums[...] = total


def spread_kernel(recv, gates, maxima):
    num, rows, _ = recv.shape
    tiles = rows // ROWS - 1
    share = tiles * LANES
    for d in range(num):
        codes = decoded(recv[d, 0 : tiles * ROWS, :])
        for j in range(tiles):
            tile = codes[j * ROWS : (j + 1) * ROWS]
            cols = slice(d * share + j * LANES, d * share + (j + 1) * LANES)
            gates[:, cols] = tile[0:TOP] * step_scale(tile[TOP : TOP + 1])
            maxima[:, cols] = fourth(unit(tile[TOP + 1 : TOP + 2]))


def balance_kernel(num_devices, per_device, total_tokens, where, own, first, second, third, out, slots):
    place = where[0]
    for k, part in enumerate((own, first, second, third)):
        slots[(place + 4 - k) % 4] = part[...]
    total = (slots[0] + slots[1]) + (slots[2] + slots[3])
    num_experts = num_devices * per_device
    prob = jnp.concatenate([total[0:1], total[1:2]], axis=1)[:, :num_experts] / total_tokens
    freq = jnp.concatenate([total[2:3], total[3:4]], axis=1)[:, :num_experts] * (
        num_experts / (TOP * total_tokens)
    )
    sent = total[4:5, :num_devices] * (num_devices / (DEV_TOP * total_tokens))

    def by_device(x):
        return functools.reduce(
            jnp.add, [x[:, j * num_devices : (j + 1) * num_devices] for j in range(per_device)]
        )

    dev_prob = by_device(prob)
    dev_freq = by_device(freq) / per_device
    losses = [jnp.sum(a * b, axis=1, keepdims=True) for a, b in ((freq, prob), (dev_freq, dev_prob), (sent, dev_prob))]
    lane = lax.broadcasted_iota(jnp.int32, (1, LANES), 1)
    out[...] = jnp.where(lane == 0, losses[0], jnp.where(lane == 1, losses[1], losses[2]))


def local(tokens, router, device_pick, expert_pick):
    features, share = tokens.shape
    num_devices = lax.axis_size(EXPERT)
    per_device = router.shape[1]
    num_experts = per_device * num_devices
    total_tokens = share * num_devices * lax.axis_size(DP)
    my_index = lax.axis_index(EXPERT)
    core, z, y = (lax.axis_index(axis) for axis in ("dp_1", "expert_0", "expert_1"))
    deep, wide = sizes = (lax.axis_size("expert_0"), lax.axis_size("expert_1"))
    group = num_devices // 2

    block = router.T.reshape(per_device * features // LANES, LANES)
    pieces = [block]
    for k in range(1, deep // 2):
        pairs = [(i, (i + k) % deep) for i in range(deep)]
        pairs += [(deep + i, deep + (i - k) % deep) for i in range(deep)]
        pieces.append(lax.ppermute(block, ("dp_1", "expert_0"), pairs))
    across = lax.ppermute(
        block, ("dp_1", "expert_0"), [(deep + i, deep + (i + deep // 2) % deep) for i in range(deep)]
    )
    pieces[0] = jnp.where(core == 0, block, across)
    column = jnp.stack(pieces)
    plane = [column] + [
        lax.ppermute(column, "expert_1", [(i, (i + k) % wide) for i in range(wide)]) for k in range(1, wide)
    ]
    own = jnp.stack(plane).reshape(group, per_device, features).transpose(1, 0, 2)
    own = own.reshape(num_experts // 2, features)
    other = lax.ppermute(own, "dp_1", [(0, 1), (1, 0)])

    steps = share // BLOCK
    where = jnp.stack([my_index, core, z, y]).astype(jnp.int32)
    rows = (share // LANES + 1) * ROWS
    msg = pl.pallas_call(
        functools.partial(route_kernel, sizes, per_device),
        out_shape=jax.ShapeDtypeStruct((num_devices, rows, LANES), jnp.int16),
        grid_spec=pltpu.PrefetchScalarGridSpec(
            num_scalar_prefetch=1,
            grid=(steps,),
            in_specs=[
                pl.BlockSpec((num_experts // 2, features), lambda i, w: (0, 0)),
                pl.BlockSpec((num_experts // 2, features), lambda i, w: (0, 0)),
                pl.BlockSpec((features, BLOCK), lambda i, w: (0, i)),
                pl.BlockSpec((TOP, BLOCK), lambda i, w: (0, w[0] * steps + i)),
                pl.BlockSpec((DEV_TOP, BLOCK), lambda i, w: (0, w[0] * steps + i)),
            ],
            out_specs=pl.BlockSpec((num_devices, rows, LANES), lambda i, w: (0, 0, 0)),
            scratch_shapes=[
                pltpu.VMEM((num_experts, features), jnp.bfloat16),
                pltpu.VMEM((num_experts, LANES), jnp.float32),
                pltpu.VMEM((num_experts, LANES), jnp.float32),
                pltpu.VMEM((num_devices, LANES), jnp.float32),
            ],
        ),
        compiler_params=pltpu.CompilerParams(
            dimension_semantics=("arbitrary",), vmem_limit_bytes=51 * 1024 * 1024
        ),
        name="route",
    )(where, own, other, tokens, expert_pick, device_pick)

    recv = lax.all_to_all(msg, EXPERT, 0, 0, tiled=True)
    sums = pl.pallas_call(
        functools.partial(sums_kernel, share),
        out_shape=jax.ShapeDtypeStruct((ROWS, LANES), jnp.float32),
        grid=(1,),
        in_specs=[pl.BlockSpec((num_devices, ROWS, LANES), lambda i: (0, rows // ROWS - 1, 0))],
        out_specs=pl.BlockSpec((ROWS, LANES), lambda i: (0, 0)),
        compiler_params=pltpu.CompilerParams(vmem_limit_bytes=2 * 1024 * 1024),
        name="sums",
    )(recv)
    gates, device_max = pl.pallas_call(
        spread_kernel,
        out_shape=(
            jax.ShapeDtypeStruct((TOP, share * num_devices), jnp.float32),
            jax.ShapeDtypeStruct((1, share * num_devices), jnp.float32),
        ),
        compiler_params=pltpu.CompilerParams(vmem_limit_bytes=16 * 1024 * 1024),
        name="spread",
    )(recv)
    chip = sums + lax.ppermute(sums, "dp_1", [(0, 1), (1, 0)])
    length = lax.axis_size("dp_0")
    others = [
        lax.ppermute(chip, "dp_0", [(i, (i + k) % length) for i in range(length)]) for k in range(1, length)
    ]
    balance = pl.pallas_call(
        functools.partial(balance_kernel, num_devices, per_device, total_tokens),
        out_shape=jax.ShapeDtypeStruct((1, LANES), jnp.float32),
        grid_spec=pltpu.PrefetchScalarGridSpec(
            num_scalar_prefetch=1,
            grid=(1,),
            in_specs=[pl.BlockSpec((ROWS, LANES), lambda i, w: (0, 0))] * 4,
            out_specs=pl.BlockSpec((1, LANES), lambda i, w: (0, 0)),
            scratch_shapes=[pltpu.VMEM((4, ROWS, LANES), jnp.float32)],
        ),
        compiler_params=pltpu.CompilerParams(vmem_limit_bytes=1024 * 1024),
        name="balance",
    )(lax.axis_index("dp_0").astype(jnp.int32).reshape(1), chip, *others)
    return (gates, device_max, balance[0, 0:3])


def solution(mesh):
    torus = Mesh(mesh.devices.reshape(4, 2, 8, 4), ("dp_0", "dp_1", "expert_0", "expert_1"))
    return jax.shard_map(
        local,
        mesh=torus,
        in_specs=(P(None, DP_EXPERT), P(None, EXPERT), P(None, DP), P(None, DP)),
        out_specs=(P(None, DP), P(EXPERT, DP), P()),
        check_vma=False,
    )
```

```python
import functools

import jax
import jax.numpy as jnp
from jax import lax
from jax.experimental import pallas as pl
from jax.experimental.pallas import tpu as pltpu
from jax.sharding import Mesh
from jax.sharding import PartitionSpec as P

TOP = 6
DEV_TOP = 3
EXPERT = ("expert_0", "expert_1")
DP = ("dp_0", "dp_1")
DP_EXPERT = ("dp_0", "dp_1", "expert_0", "expert_1")
BLOCK = 256
LANES = 128
ROWS = 8
TOP_CODE = 65535.0
MIDDLE = 32768
TINY = 1e-30


def sent_to_all(x, axis):
    length = lax.axis_size(axis)
    return lax.all_to_all(jnp.broadcast_to(x[None], (length, *x.shape)), axis, 0, 0, tiled=True)


def lane_sum(x):
    parts = [x[:, i : i + LANES] for i in range(0, x.shape[1], LANES)]
    return functools.reduce(jnp.add, parts)


def fourth(x):
    return jnp.square(jnp.square(x))


def eighth(x):
    return jnp.square(fourth(x))


def eighth_root(x):
    return jnp.sqrt(jnp.sqrt(jnp.sqrt(x)))


def unit(code):
    return code * (1.0 / TOP_CODE)


def step_scale(code):
    return jnp.maximum(eighth(unit(code)), TINY) * (1.0 / TOP_CODE)


def source_device(core, place, row, half, sizes):
    deep, wide = sizes
    z, y = place
    back = row % (deep // 2)
    aside = (row // (deep // 2)) % wide
    ahead = jnp.where(back == 0, deep // 2, back)
    offset = jnp.where(core == half, deep - back, ahead)
    return ((z + offset) % deep) * wide + (y + wide - aside) % wide


def route_kernel(
    sizes, per_device, where, own, other, tokens, picks, devs, out, sums, router, prob_acc, count_acc, sent_acc
):
    step = pl.program_id(0)
    deep, wide = sizes
    num_devices = deep * wide
    num_experts = num_devices * per_device
    group = num_devices // 2
    rows_half = num_experts // 2
    block = tokens.shape[1]
    tiles = block // LANES
    core, place = where[0], (where[1], where[2])

    @pl.when(step == 0)
    def _():
        router[:rows_half] = own[...]
        router[rows_half:] = other[...]
        prob_acc[...] = jnp.zeros_like(prob_acc)
        count_acc[...] = jnp.zeros_like(count_acc)
        sent_acc[...] = jnp.zeros_like(sent_acc)

    row = lax.broadcasted_iota(jnp.int32, (num_experts, LANES), 0)
    half = row // rows_half
    dev = source_device(core, place, row % group, half, sizes)
    slot = (row % rows_half) // group
    ids = dev * per_device + slot
    ids_wide = jnp.concatenate([ids] * tiles, axis=1)

    scores = jnp.dot(router[...], tokens[...], preferred_element_type=jnp.float32)
    peak = jnp.max(scores, axis=0, keepdims=True)
    raised = jnp.exp(scores - peak)
    probs = raised / jnp.sum(raised, axis=0, keepdims=True)
    prob_acc[...] += lane_sum(probs)
    chosen = []
    hits = jnp.zeros((num_experts, block), jnp.float32)
    for k in range(TOP):
        mask = ids_wide == picks[k : k + 1, :]
        chosen.append(jnp.sum(jnp.where(mask, probs, 0.0), axis=0, keepdims=True))
        hits += jnp.where(mask, 1.0, 0.0)
    count_acc[...] += lane_sum(hits)
    dev_ids = lax.broadcasted_iota(jnp.int32, (num_devices, block), 0)
    sent = jnp.zeros((num_devices, block), jnp.float32)
    for k in range(DEV_TOP):
        sent += jnp.where(dev_ids == devs[k : k + 1, :], 1.0, 0.0)
    sent_acc[...] += lane_sum(sent)

    largest = functools.reduce(jnp.maximum, chosen)
    scale = jnp.minimum(jnp.floor(eighth_root(largest) * TOP_CODE) + 1.0, TOP_CODE)
    inverse = 1.0 / step_scale(scale)
    codes = [jnp.minimum(jnp.round(g * inverse), TOP_CODE) for g in chosen]
    lines = jnp.concatenate([*codes, scale, scale], axis=0).astype(jnp.int32) - MIDDLE
    stacked = jnp.concatenate([lines[:, j * LANES : (j + 1) * LANES] for j in range(tiles)], axis=0)
    last = lax.broadcasted_iota(jnp.int32, stacked.shape, 0) % ROWS == ROWS - 1
    here = pl.ds(pl.multiple_of(step * tiles * ROWS, tiles * ROWS), tiles * ROWS)
    for h in range(2):
        slabs = [probs[h * rows_half + j * group : h * rows_half + (j + 1) * group] for j in range(per_device)]
        maxima = functools.reduce(jnp.maximum, slabs)
        max_codes = jnp.round(jnp.sqrt(jnp.sqrt(maxima)) * TOP_CODE).astype(jnp.int32) - MIDDLE
        max_codes = jnp.minimum(max_codes, MIDDLE - 1)
        for s in range(group):
            line = jnp.concatenate(
                [
                    jnp.broadcast_to(max_codes[s : s + 1, j * LANES : (j + 1) * LANES], (ROWS, LANES))
                    for j in range(tiles)
                ],
                axis=0,
            )
            target = source_device(core, place, s, h, sizes)
            out[target, here, :] = jnp.where(last, line, stacked).astype(jnp.int16)

    @pl.when(step == pl.num_programs(0) - 1)
    def _():
        def lined(acc, index):
            total = jnp.sum(acc[...], axis=1, keepdims=True)
            lanes = lax.broadcasted_iota(jnp.int32, index.shape, 1)
            parts = [
                jnp.sum(jnp.where(index == lanes + i * LANES, total, 0.0), axis=0, keepdims=True) for i in range(2)
            ]
            return parts

        order = slot * num_devices + dev
        device_rows = lax.broadcasted_iota(jnp.int32, (num_devices, LANES), 0)
        parts = [*lined(prob_acc, order), *lined(count_acc, order), *lined(sent_acc, device_rows)]
        sums[...] = jnp.concatenate([*parts, jnp.zeros((ROWS - len(parts), LANES), jnp.float32)], axis=0)


def decoded(codes):
    return codes.astype(jnp.int32).astype(jnp.float32) + float(MIDDLE)


def spread_kernel(recv, gates, maxima):
    num, rows, _ = recv.shape
    tiles = rows // ROWS
    share = tiles * LANES
    for d in range(num):
        codes = decoded(recv[d, 0 : tiles * ROWS, :])
        for j in range(tiles):
            tile = codes[j * ROWS : (j + 1) * ROWS]
            cols = slice(d * share + j * LANES, d * share + (j + 1) * LANES)
            gates[:, cols] = tile[0:TOP] * step_scale(tile[TOP : TOP + 1])
            maxima[:, cols] = fourth(unit(tile[TOP + 1 : TOP + 2]))


def ring_sum_kernel(where, own, first, second, third, out, slots):
    place = where[0]
    for k, part in enumerate((own, first, second, third)):
        slots[(place + 4 - k) % 4] = part[...]
    out[...] = (slots[0] + slots[1]) + (slots[2] + slots[3])


def ring_slots_kernel(where, own, first, second, third, across, out):
    core, z = where[0], where[1]
    out[...] = jnp.zeros_like(out)
    for k, part in enumerate((first, second, third), 1):
        out[(z + jnp.where(core == 0, 8 - k, k)) % 8] = part[...]
    near = jnp.where(core == 0, own[...], across[...])
    out[(z + jnp.where(core == 0, 0, 4)) % 8] = near


def balance_kernel(num_devices, per_device, total_tokens, mine, others, out):
    total = functools.reduce(jnp.add, [mine[i] + others[i] for i in range(8)])
    num_experts = num_devices * per_device
    prob = jnp.concatenate([total[0:1], total[1:2]], axis=1)[:, :num_experts] / total_tokens
    freq = jnp.concatenate([total[2:3], total[3:4]], axis=1)[:, :num_experts] * (
        num_experts / (TOP * total_tokens)
    )
    sent = total[4:5, :num_devices] * (num_devices / (DEV_TOP * total_tokens))

    def by_device(x):
        return functools.reduce(
            jnp.add, [x[:, j * num_devices : (j + 1) * num_devices] for j in range(per_device)]
        )

    dev_prob = by_device(prob)
    dev_freq = by_device(freq) / per_device
    losses = [jnp.sum(a * b, axis=1, keepdims=True) for a, b in ((freq, prob), (dev_freq, dev_prob), (sent, dev_prob))]
    lane = lax.broadcasted_iota(jnp.int32, (1, LANES), 1)
    out[...] = jnp.where(lane == 0, losses[0], jnp.where(lane == 1, losses[1], losses[2]))


def along_z(x, deep):
    axes = ("dp_1", "expert_0")
    parts = []
    for k in range(1, deep // 2):
        pairs = [(i, (i + k) % deep) for i in range(deep)]
        pairs += [(deep + i, deep + (i - k) % deep) for i in range(deep)]
        parts.append(lax.ppermute(x, axes, pairs))
    far = [(deep + i, deep + (i + deep // 2) % deep) for i in range(deep)]
    return (*parts, lax.ppermute(x, axes, far))


def local(tokens, router, device_pick, expert_pick):
    features, share = tokens.shape
    num_devices = lax.axis_size(EXPERT)
    per_device = router.shape[1]
    num_experts = per_device * num_devices
    total_tokens = share * num_devices * lax.axis_size(DP)
    my_index = lax.axis_index(EXPERT)
    core, z, y = (lax.axis_index(axis) for axis in ("dp_1", "expert_0", "expert_1"))
    deep, wide = sizes = (lax.axis_size("expert_0"), lax.axis_size("expert_1"))
    group = num_devices // 2

    block = router.T.reshape(per_device * features // LANES, LANES)
    *pieces, across = along_z(block, deep)
    pieces = [jnp.where(core == 0, block, across), *pieces]
    column = jnp.stack(pieces)
    plane = [column] + [
        lax.ppermute(column, "expert_1", [(i, (i + k) % wide) for i in range(wide)]) for k in range(1, wide)
    ]
    own = jnp.stack(plane).reshape(group, per_device, features).transpose(1, 0, 2)
    own = own.reshape(num_experts // 2, features)
    other = lax.ppermute(own, "dp_1", [(0, 1), (1, 0)])

    steps = share // BLOCK
    where = jnp.stack([core, z, y]).astype(jnp.int32)
    rows = share // LANES * ROWS
    experts_here = lax.dynamic_slice_in_dim(expert_pick, my_index * share, share, 1)
    devices_here = lax.dynamic_slice_in_dim(device_pick, my_index * share, share, 1)
    msg, sums = pl.pallas_call(
        functools.partial(route_kernel, sizes, per_device),
        out_shape=(
            jax.ShapeDtypeStruct((num_devices, rows, LANES), jnp.int16),
            jax.ShapeDtypeStruct((ROWS, LANES), jnp.float32),
        ),
        grid_spec=pltpu.PrefetchScalarGridSpec(
            num_scalar_prefetch=1,
            grid=(steps,),
            in_specs=[
                pl.BlockSpec((num_experts // 2, features), lambda i, w: (0, 0)),
                pl.BlockSpec((num_experts // 2, features), lambda i, w: (0, 0)),
                pl.BlockSpec((features, BLOCK), lambda i, w: (0, i)),
                pl.BlockSpec((TOP, BLOCK), lambda i, w: (0, i)),
                pl.BlockSpec((DEV_TOP, BLOCK), lambda i, w: (0, i)),
            ],
            out_specs=(
                pl.BlockSpec((num_devices, rows, LANES), lambda i, w: (0, 0, 0)),
                pl.BlockSpec((ROWS, LANES), lambda i, w: (0, 0)),
            ),
            scratch_shapes=[
                pltpu.VMEM((num_experts, features), jnp.bfloat16),
                pltpu.VMEM((num_experts, LANES), jnp.float32),
                pltpu.VMEM((num_experts, LANES), jnp.float32),
                pltpu.VMEM((num_devices, LANES), jnp.float32),
            ],
        ),
        compiler_params=pltpu.CompilerParams(
            dimension_semantics=("arbitrary",), vmem_limit_bytes=51 * 1024 * 1024
        ),
        name="route",
    )(where, own, other, tokens, experts_here, devices_here)

    recv = lax.all_to_all(msg, EXPERT, 0, 0, tiled=True)
    gates, device_max = pl.pallas_call(
        spread_kernel,
        out_shape=(
            jax.ShapeDtypeStruct((TOP, share * num_devices), jnp.float32),
            jax.ShapeDtypeStruct((1, share * num_devices), jnp.float32),
        ),
        compiler_params=pltpu.CompilerParams(vmem_limit_bytes=16 * 1024 * 1024),
        name="spread",
    )(recv)

    small = pltpu.CompilerParams(vmem_limit_bytes=1024 * 1024)
    tile = pl.BlockSpec((ROWS, LANES), lambda i, w: (0, 0))
    scalar = lambda *values: jnp.stack(values).astype(jnp.int32)

    def summed(x, axis):
        length = lax.axis_size(axis)
        others = [lax.ppermute(x, axis, [(i, (i + k) % length) for i in range(length)]) for k in range(1, length)]
        return pl.pallas_call(
            ring_sum_kernel,
            out_shape=jax.ShapeDtypeStruct((ROWS, LANES), jnp.float32),
            grid_spec=pltpu.PrefetchScalarGridSpec(
                num_scalar_prefetch=1,
                grid=(1,),
                in_specs=[tile] * length,
                out_specs=tile,
                scratch_shapes=[pltpu.VMEM((length, ROWS, LANES), jnp.float32)],
            ),
            compiler_params=small,
            name="ring_sum",
        )(scalar(lax.axis_index(axis)), x, *others)

    sums = sums + lax.ppermute(sums, "dp_1", [(0, 1), (1, 0)])
    sums = summed(summed(sums, "dp_0"), "expert_1")
    mine = pl.pallas_call(
        ring_slots_kernel,
        out_shape=jax.ShapeDtypeStruct((deep, ROWS, LANES), jnp.float32),
        grid_spec=pltpu.PrefetchScalarGridSpec(
            num_scalar_prefetch=1,
            grid=(1,),
            in_specs=[tile] * 5,
            out_specs=pl.BlockSpec((deep, ROWS, LANES), lambda i, w: (0, 0, 0)),
        ),
        compiler_params=small,
        name="ring_slots",
    )(scalar(core, z), sums, *along_z(sums, deep))
    balance = pl.pallas_call(
        functools.partial(balance_kernel, num_devices, per_device, total_tokens),
        out_shape=jax.ShapeDtypeStruct((1, LANES), jnp.float32),
        compiler_params=small,
        name="balance",
    )(mine, lax.ppermute(mine, "dp_1", [(0, 1), (1, 0)]))
    return (gates, device_max, balance[0, 0:3])


def solution(mesh):
    torus = Mesh(mesh.devices.reshape(4, 2, 8, 4), ("dp_0", "dp_1", "expert_0", "expert_1"))
    return jax.shard_map(
        local,
        mesh=torus,
        in_specs=(P(None, DP_EXPERT), P(None, EXPERT), P(None, DP), P(None, DP)),
        out_specs=(P(None, DP), P(EXPERT, DP), P()),
        check_vma=False,
    )
```

```python
import functools

import jax
import jax.numpy as jnp
from jax import lax
from jax.experimental import pallas as pl
from jax.experimental.pallas import tpu as pltpu
from jax.sharding import Mesh
from jax.sharding import PartitionSpec as P

TOP = 6
DEV_TOP = 3
EXPERT = ("expert_0", "expert_1")
DP = ("dp_0", "dp_1")
DP_EXPERT = ("dp_0", "dp_1", "expert_0", "expert_1")
BLOCK = 256
PIECES = 1
LANES = 128
ROWS = 8
TOP_CODE = 65535.0
MIDDLE = 32768
TINY = 1e-30


def sent_to_all(x, axis):
    length = lax.axis_size(axis)
    return lax.all_to_all(jnp.broadcast_to(x[None], (length, *x.shape)), axis, 0, 0, tiled=True)


def lane_sum(x):
    parts = [x[:, i : i + LANES] for i in range(0, x.shape[1], LANES)]
    return functools.reduce(jnp.add, parts)


def fourth(x):
    return jnp.square(jnp.square(x))


def eighth(x):
    return jnp.square(fourth(x))


def eighth_root(x):
    return jnp.sqrt(jnp.sqrt(jnp.sqrt(x)))


def unit(code):
    return code * (1.0 / TOP_CODE)


def step_scale(code):
    return jnp.maximum(eighth(unit(code)), TINY) * (1.0 / TOP_CODE)


def coded_pair(x, limit):
    coarse = jnp.minimum(jnp.floor(eighth_root(x * (1.0 / limit)) * TOP_CODE), TOP_CODE)
    base = eighth(unit(coarse)) * limit
    rest = jnp.where(base > 0.0, (x - base) / jnp.maximum(base, TINY), 0.0)
    fine = jnp.round(jnp.clip(rest * coarse * (1.0 / 16.0), 0.0, 1.0) * TOP_CODE)
    return coarse, fine


def decoded_pair(coarse, fine, limit):
    base = eighth(unit(coarse)) * limit
    return base * (1.0 + unit(fine) * 16.0 / jnp.maximum(coarse, 1.0))


def source_devices(core, place, sizes):
    deep, wide = sizes
    z, y = place
    row = jnp.arange(deep * wide, dtype=jnp.int32)
    back = row % (deep // 2)
    aside = (row // (deep // 2)) % wide
    half = row // (deep * wide // 2)
    ahead = jnp.where(back == 0, deep // 2, back)
    offset = jnp.where(core == half, deep - back, ahead)
    return ((z + offset) % deep) * wide + (y + wide - aside) % wide


def lined(total, index):
    lanes = lax.broadcasted_iota(jnp.int32, index.shape, 1)
    return [
        jnp.sum(jnp.where(index == lanes + i * LANES, total, 0.0), axis=0, keepdims=True) for i in range(2)
    ]


def count_kernel(num_devices, per_device, picks, devs, out):
    num_experts = num_devices * per_device
    share = picks.shape[1]
    counts, sent = [], []
    for j in range(per_device):
        ids = lax.broadcasted_iota(jnp.int32, (num_devices, LANES), 0) * per_device + j
        total = jnp.zeros((num_devices, LANES), jnp.float32)
        for c in range(0, share, LANES):
            for k in range(TOP):
                total += jnp.where(ids == picks[k : k + 1, c : c + LANES], 1.0, 0.0)
        counts.append(jnp.sum(total, axis=1, keepdims=True))
    ids = lax.broadcasted_iota(jnp.int32, (num_devices, LANES), 0)
    total = jnp.zeros((num_devices, LANES), jnp.float32)
    for c in range(0, share, LANES):
        for k in range(DEV_TOP):
            total += jnp.where(ids == devs[k : k + 1, c : c + LANES], 1.0, 0.0)
    rows = lax.broadcasted_iota(jnp.int32, (num_experts, LANES), 0)
    low, high = lined(jnp.concatenate(counts, axis=0), rows)
    sent_low, sent_high = lined(jnp.sum(total, axis=1, keepdims=True), ids)
    none = jnp.zeros((ROWS - 4, LANES), jnp.float32)
    out[...] = jnp.concatenate([low, high, sent_low, sent_high, none], axis=0)


def route_kernel(
    num_devices, per_device, where, own, other, tokens, picks, counts, out, router, ids, blocks, arrived, prob_acc
):
    step = pl.program_id(0)
    num_experts = num_devices * per_device
    group = num_devices // 2
    rows_half = num_experts // 2
    steps, features, block = blocks.shape
    tiles = block // LANES
    share = block * steps
    depth = features // PIECES

    def piece(i, p):
        rows = pl.ds(p * depth, depth)
        cols = pl.ds(i * block, block)
        return pltpu.make_async_copy(tokens.at[rows, cols], blocks.at[i, rows, :], arrived.at[i, p])

    @pl.when(step == 0)
    def _():
        for i in range(steps):
            for p in range(PIECES):
                piece(i, p).start()
        router[:rows_half] = own[...]
        router[rows_half:] = other[...]
        prob_acc[...] = jnp.zeros_like(prob_acc)
        row = lax.broadcasted_iota(jnp.int32, (group, LANES), 0)
        for h in range(2):
            dev = jnp.zeros((group, LANES), jnp.int32)
            for s in range(group):
                dev = jnp.where(row == s, where[h * group + s], dev)
            for j in range(per_device):
                ids[pl.ds(h * rows_half + j * group, group), :] = dev * per_device + j

    for p in range(PIECES):
        piece(step, p).wait()
    scores = jnp.dot(router[...], blocks[step], preferred_element_type=jnp.float32)
    peak = jnp.max(scores, axis=0, keepdims=True)
    raised = jnp.exp(scores - peak)
    probs = raised * (1.0 / jnp.sum(raised, axis=0, keepdims=True))
    prob_acc[...] += lane_sum(probs)
    ids_wide = jnp.concatenate([ids[...]] * tiles, axis=1)
    chosen = [
        jnp.sum(jnp.where(ids_wide == picks[k : k + 1, :], probs, 0.0), axis=0, keepdims=True)
        for k in range(TOP)
    ]

    largest = functools.reduce(jnp.maximum, chosen)
    scale = jnp.minimum(jnp.floor(eighth_root(largest) * TOP_CODE) + 1.0, TOP_CODE)
    inverse = 1.0 / step_scale(scale)
    codes = [jnp.minimum(jnp.round(g * inverse), TOP_CODE) for g in chosen]
    lines = jnp.concatenate([*codes, scale, scale], axis=0).astype(jnp.int32) - MIDDLE
    stacked = jnp.concatenate([lines[:, j * LANES : (j + 1) * LANES] for j in range(tiles)], axis=0)
    last = (lax.broadcasted_iota(jnp.int32, stacked.shape, 0) & (ROWS - 1)) == ROWS - 1
    here = pl.ds(pl.multiple_of(step * tiles * ROWS, tiles * ROWS), tiles * ROWS)
    for h in range(2):
        slabs = [probs[h * rows_half + j * group : h * rows_half + (j + 1) * group] for j in range(per_device)]
        maxima = functools.reduce(jnp.maximum, slabs)
        max_codes = jnp.round(jnp.sqrt(jnp.sqrt(maxima)) * TOP_CODE).astype(jnp.int32) - MIDDLE
        max_codes = jnp.minimum(max_codes, MIDDLE - 1)
        for s in range(group):
            line = jnp.concatenate(
                [
                    jnp.broadcast_to(max_codes[s : s + 1, j * LANES : (j + 1) * LANES], (ROWS, LANES))
                    for j in range(tiles)
                ],
                axis=0,
            )
            out[where[h * group + s], here, :] = jnp.where(last, line, stacked).astype(jnp.int16)

    @pl.when(step == steps - 1)
    def _():
        expert = ids[...]
        dev = jnp.zeros_like(expert)
        for d in range(1, num_devices):
            dev += jnp.where(expert >= d * per_device, 1, 0)
        order = (expert - dev * per_device) * num_devices + dev
        low, high = lined(jnp.sum(prob_acc[...], axis=1, keepdims=True), order)
        low_coarse, low_fine = coded_pair(low, share)
        high_coarse, high_fine = coded_pair(high, share)
        sums = jnp.concatenate([low_coarse, high_coarse, low_fine, high_fine, counts[0:4, :]], axis=0)
        sums = (sums.astype(jnp.int32) - MIDDLE).astype(jnp.int16)
        for d in range(num_devices):
            out[d, pl.ds(share // LANES * ROWS, ROWS), :] = sums


def route(num_devices, per_device, where, own, other, tokens, picks, counts):
    features, share = tokens.shape
    num_experts = num_devices * per_device
    rows = (share // LANES + 1) * ROWS
    steps = share // BLOCK
    return pl.pallas_call(
        functools.partial(route_kernel, num_devices, per_device),
        out_shape=jax.ShapeDtypeStruct((num_devices, rows, LANES), jnp.int16),
        grid_spec=pltpu.PrefetchScalarGridSpec(
            num_scalar_prefetch=1,
            grid=(steps,),
            in_specs=[
                pl.BlockSpec((num_experts // 2, features), lambda i, w: (0, 0)),
                pl.BlockSpec((num_experts // 2, features), lambda i, w: (0, 0)),
                pl.BlockSpec(memory_space=pl.ANY),
                pl.BlockSpec((TOP, BLOCK), lambda i, w: (0, i)),
                pl.BlockSpec((ROWS, LANES), lambda i, w: (0, 0)),
            ],
            out_specs=pl.BlockSpec((num_devices, rows, LANES), lambda i, w: (0, 0, 0)),
            scratch_shapes=[
                pltpu.VMEM((num_experts, features), jnp.bfloat16),
                pltpu.VMEM((num_experts, LANES), jnp.int32),
                pltpu.VMEM((steps, features, BLOCK), jnp.bfloat16),
                pltpu.SemaphoreType.DMA((steps, PIECES)),
                pltpu.VMEM((num_experts, LANES), jnp.float32),
            ],
        ),
        compiler_params=pltpu.CompilerParams(
            dimension_semantics=("arbitrary",), vmem_limit_bytes=51 * 1024 * 1024
        ),
        name="route",
    )(where, own, other, tokens, picks, counts)


def decoded(codes):
    return codes.astype(jnp.int32).astype(jnp.float32) + float(MIDDLE)


def sums_kernel(share, recv, sums):
    total = jnp.zeros((ROWS, LANES), jnp.float32)
    for d in range(recv.shape[0]):
        tile = decoded(recv[d])
        probs = decoded_pair(tile[0:2], tile[2:4], share)
        total += jnp.concatenate([probs, tile[4:8], jnp.zeros((2, LANES), jnp.float32)], axis=0)
    sums[...] = total


def spread_kernel(recv, gates, maxima):
    num, rows, _ = recv.shape
    tiles = rows // ROWS - 1
    share = tiles * LANES
    for d in range(num):
        codes = decoded(recv[d, 0 : tiles * ROWS, :])
        for j in range(tiles):
            tile = codes[j * ROWS : (j + 1) * ROWS]
            cols = slice(d * share + j * LANES, d * share + (j + 1) * LANES)
            gates[:, cols] = tile[0:TOP] * step_scale(tile[TOP : TOP + 1])
            maxima[:, cols] = fourth(unit(tile[TOP + 1 : TOP + 2]))


def balance_kernel(num_devices, per_device, total_tokens, where, own, first, second, third, out, slots):
    place = where[0]
    for k, part in enumerate((own, first, second, third)):
        slots[(place + 4 - k) % 4] = part[...]
    total = (slots[0] + slots[1]) + (slots[2] + slots[3])
    num_experts = num_devices * per_device
    prob = jnp.concatenate([total[0:1], total[1:2]], axis=1)[:, :num_experts] / total_tokens
    freq = jnp.concatenate([total[2:3], total[3:4]], axis=1)[:, :num_experts] * (
        num_experts / (TOP * total_tokens)
    )
    sent = total[4:5, :num_devices] * (num_devices / (DEV_TOP * total_tokens))

    def by_device(x):
        return functools.reduce(
            jnp.add, [x[:, j * num_devices : (j + 1) * num_devices] for j in range(per_device)]
        )

    dev_prob = by_device(prob)
    dev_freq = by_device(freq) / per_device
    losses = [jnp.sum(a * b, axis=1, keepdims=True) for a, b in ((freq, prob), (dev_freq, dev_prob), (sent, dev_prob))]
    lane = lax.broadcasted_iota(jnp.int32, (1, LANES), 1)
    out[...] = jnp.where(lane == 0, losses[0], jnp.where(lane == 1, losses[1], losses[2]))


def local(tokens, router, device_pick, expert_pick):
    features, share = tokens.shape
    num_devices = lax.axis_size(EXPERT)
    per_device = router.shape[1]
    num_experts = per_device * num_devices
    total_tokens = share * num_devices * lax.axis_size(DP)
    my_index = lax.axis_index(EXPERT)
    core, z, y = (lax.axis_index(axis) for axis in ("dp_1", "expert_0", "expert_1"))
    deep, wide = sizes = (lax.axis_size("expert_0"), lax.axis_size("expert_1"))
    group = num_devices // 2

    block = router.T.reshape(per_device * features // LANES, LANES)
    pieces = [block]
    for k in range(1, deep // 2):
        pairs = [(i, (i + k) % deep) for i in range(deep)]
        pairs += [(deep + i, deep + (i - k) % deep) for i in range(deep)]
        pieces.append(lax.ppermute(block, ("dp_1", "expert_0"), pairs))
    across = lax.ppermute(
        block, ("dp_1", "expert_0"), [(deep + i, deep + (i + deep // 2) % deep) for i in range(deep)]
    )
    pieces[0] = jnp.where(core == 0, block, across)
    column = jnp.stack(pieces)
    plane = [column] + [
        lax.ppermute(column, "expert_1", [(i, (i + k) % wide) for i in range(wide)]) for k in range(1, wide)
    ]
    own = jnp.stack(plane).reshape(group, per_device, features).transpose(1, 0, 2)
    own = own.reshape(num_experts // 2, features)
    other = lax.ppermute(own, "dp_1", [(0, 1), (1, 0)])

    where = source_devices(core, (z, y), sizes)
    rows = (share // LANES + 1) * ROWS
    experts_here = lax.dynamic_slice_in_dim(expert_pick, my_index * share, share, 1)
    devices_here = lax.dynamic_slice_in_dim(device_pick, my_index * share, share, 1)
    counts = pl.pallas_call(
        functools.partial(count_kernel, num_devices, per_device),
        out_shape=jax.ShapeDtypeStruct((ROWS, LANES), jnp.float32),
        compiler_params=pltpu.CompilerParams(vmem_limit_bytes=2 * 1024 * 1024),
        name="count",
    )(experts_here, devices_here)
    msg = route(num_devices, per_device, where, own, other, tokens, experts_here, counts)

    recv = lax.all_to_all(msg, EXPERT, 0, 0, tiled=True)
    sums = pl.pallas_call(
        functools.partial(sums_kernel, share),
        out_shape=jax.ShapeDtypeStruct((ROWS, LANES), jnp.float32),
        grid=(1,),
        in_specs=[pl.BlockSpec((num_devices, ROWS, LANES), lambda i: (0, rows // ROWS - 1, 0))],
        out_specs=pl.BlockSpec((ROWS, LANES), lambda i: (0, 0)),
        compiler_params=pltpu.CompilerParams(vmem_limit_bytes=2 * 1024 * 1024),
        name="sums",
    )(recv)
    gates, device_max = pl.pallas_call(
        spread_kernel,
        out_shape=(
            jax.ShapeDtypeStruct((TOP, share * num_devices), jnp.float32),
            jax.ShapeDtypeStruct((1, share * num_devices), jnp.float32),
        ),
        compiler_params=pltpu.CompilerParams(vmem_limit_bytes=16 * 1024 * 1024),
        name="spread",
    )(recv)
    chip = sums + lax.ppermute(sums, "dp_1", [(0, 1), (1, 0)])
    length = lax.axis_size("dp_0")
    others = [
        lax.ppermute(chip, "dp_0", [(i, (i + k) % length) for i in range(length)]) for k in range(1, length)
    ]
    balance = pl.pallas_call(
        functools.partial(balance_kernel, num_devices, per_device, total_tokens),
        out_shape=jax.ShapeDtypeStruct((1, LANES), jnp.float32),
        grid_spec=pltpu.PrefetchScalarGridSpec(
            num_scalar_prefetch=1,
            grid=(1,),
            in_specs=[pl.BlockSpec((ROWS, LANES), lambda i, w: (0, 0))] * 4,
            out_specs=pl.BlockSpec((1, LANES), lambda i, w: (0, 0)),
            scratch_shapes=[pltpu.VMEM((4, ROWS, LANES), jnp.float32)],
        ),
        compiler_params=pltpu.CompilerParams(vmem_limit_bytes=1024 * 1024),
        name="balance",
    )(lax.axis_index("dp_0").astype(jnp.int32).reshape(1), chip, *others)
    return (gates, device_max, balance[0, 0:3])


def solution(mesh):
    torus = Mesh(mesh.devices.reshape(4, 2, 8, 4), ("dp_0", "dp_1", "expert_0", "expert_1"))
    return jax.shard_map(
        local,
        mesh=torus,
        in_specs=(P(None, DP_EXPERT), P(None, EXPERT), P(None, DP), P(None, DP)),
        out_specs=(P(None, DP), P(EXPERT, DP), P()),
        check_vma=False,
    )
```

```python
import functools

import jax
import jax.numpy as jnp
from jax import lax
from jax.experimental import pallas as pl
from jax.experimental.pallas import tpu as pltpu
from jax.sharding import Mesh
from jax.sharding import PartitionSpec as P

TOP = 6
DEV_TOP = 3
EXPERT = ("expert_0", "expert_1")
DP = ("dp_0", "dp_1")
DP_EXPERT = ("dp_0", "dp_1", "expert_0", "expert_1")
BLOCK = 256
PIECES = 1
LANES = 128
ROWS = 8
TOP_CODE = 65535.0
MIDDLE = 32768
TINY = 1e-30


def sent_to_all(x, axis):
    length = lax.axis_size(axis)
    return lax.all_to_all(jnp.broadcast_to(x[None], (length, *x.shape)), axis, 0, 0, tiled=True)


def lane_sum(x):
    parts = [x[:, i : i + LANES] for i in range(0, x.shape[1], LANES)]
    return functools.reduce(jnp.add, parts)


def fourth(x):
    return jnp.square(jnp.square(x))


def eighth(x):
    return jnp.square(fourth(x))


def eighth_root(x):
    return jnp.sqrt(jnp.sqrt(jnp.sqrt(x)))


def unit(code):
    return code * (1.0 / TOP_CODE)


def step_scale(code):
    return jnp.maximum(eighth(unit(code)), TINY) * (1.0 / TOP_CODE)


def coded_pair(x, limit):
    coarse = jnp.minimum(jnp.floor(eighth_root(x * (1.0 / limit)) * TOP_CODE), TOP_CODE)
    base = eighth(unit(coarse)) * limit
    rest = jnp.where(base > 0.0, (x - base) / jnp.maximum(base, TINY), 0.0)
    fine = jnp.round(jnp.clip(rest * coarse * (1.0 / 16.0), 0.0, 1.0) * TOP_CODE)
    return coarse, fine


def decoded_pair(coarse, fine, limit):
    base = eighth(unit(coarse)) * limit
    return base * (1.0 + unit(fine) * 16.0 / jnp.maximum(coarse, 1.0))


def source_devices(core, place, sizes):
    deep, wide = sizes
    z, y = place
    row = jnp.arange(deep * wide, dtype=jnp.int32)
    back = row % (deep // 2)
    aside = (row // (deep // 2)) % wide
    half = row // (deep * wide // 2)
    ahead = jnp.where(back == 0, deep // 2, back)
    offset = jnp.where(core == half, deep - back, ahead)
    return ((z + offset) % deep) * wide + (y + wide - aside) % wide


def lined(total, index):
    lanes = lax.broadcasted_iota(jnp.int32, index.shape, 1)
    return [
        jnp.sum(jnp.where(index == lanes + i * LANES, total, 0.0), axis=0, keepdims=True) for i in range(2)
    ]


def count_kernel(num_devices, per_device, picks, devs, out):
    num_experts = num_devices * per_device
    share = picks.shape[1]
    counts, sent = [], []
    for j in range(per_device):
        ids = lax.broadcasted_iota(jnp.int32, (num_devices, LANES), 0) * per_device + j
        total = jnp.zeros((num_devices, LANES), jnp.float32)
        for c in range(0, share, LANES):
            for k in range(TOP):
                total += jnp.where(ids == picks[k : k + 1, c : c + LANES], 1.0, 0.0)
        counts.append(jnp.sum(total, axis=1, keepdims=True))
    ids = lax.broadcasted_iota(jnp.int32, (num_devices, LANES), 0)
    total = jnp.zeros((num_devices, LANES), jnp.float32)
    for c in range(0, share, LANES):
        for k in range(DEV_TOP):
            total += jnp.where(ids == devs[k : k + 1, c : c + LANES], 1.0, 0.0)
    rows = lax.broadcasted_iota(jnp.int32, (num_experts, LANES), 0)
    low, high = lined(jnp.concatenate(counts, axis=0), rows)
    sent_low, sent_high = lined(jnp.sum(total, axis=1, keepdims=True), ids)
    none = jnp.zeros((ROWS - 4, LANES), jnp.float32)
    out[...] = jnp.concatenate([low, high, sent_low, sent_high, none], axis=0)


def route_kernel(
    num_devices, per_device, where, own, other, tokens, picks, counts, out, router, ids, blocks, arrived, prob_acc
):
    step = pl.program_id(0)
    num_experts = num_devices * per_device
    group = num_devices // 2
    rows_half = num_experts // 2
    steps, features, block = blocks.shape
    tiles = block // LANES
    share = block * steps
    depth = features // PIECES

    def piece(i, p):
        rows = pl.ds(p * depth, depth)
        cols = pl.ds(i * block, block)
        return pltpu.make_async_copy(tokens.at[rows, cols], blocks.at[i, rows, :], arrived.at[i, p])

    @pl.when(step == 0)
    def _():
        for i in range(steps):
            for p in range(PIECES):
                piece(i, p).start()
        router[:rows_half] = own[...]
        router[rows_half:] = other[...]
        prob_acc[...] = jnp.zeros_like(prob_acc)
        row = lax.broadcasted_iota(jnp.int32, (group, LANES), 0)
        for h in range(2):
            dev = jnp.zeros((group, LANES), jnp.int32)
            for s in range(group):
                dev = jnp.where(row == s, where[h * group + s], dev)
            for j in range(per_device):
                ids[pl.ds(h * rows_half + j * group, group), :] = dev * per_device + j

    for p in range(PIECES):
        piece(step, p).wait()
    scores = jnp.dot(router[...], blocks[step], preferred_element_type=jnp.float32)
    peak = jnp.max(scores, axis=0, keepdims=True)
    raised = jnp.exp(scores - peak)
    probs = raised * (1.0 / jnp.sum(raised, axis=0, keepdims=True))
    prob_acc[...] += lane_sum(probs)
    ids_wide = jnp.concatenate([ids[...]] * tiles, axis=1)
    chosen = [
        jnp.sum(jnp.where(ids_wide == picks[k : k + 1, :], probs, 0.0), axis=0, keepdims=True)
        for k in range(TOP)
    ]

    largest = functools.reduce(jnp.maximum, chosen)
    scale = jnp.minimum(jnp.floor(eighth_root(largest) * TOP_CODE) + 1.0, TOP_CODE)
    inverse = 1.0 / step_scale(scale)
    codes = [jnp.minimum(jnp.round(g * inverse), TOP_CODE) for g in chosen]
    lines = jnp.concatenate([*codes, scale, scale], axis=0).astype(jnp.int32) - MIDDLE
    stacked = jnp.concatenate([lines[:, j * LANES : (j + 1) * LANES] for j in range(tiles)], axis=0)
    last = (lax.broadcasted_iota(jnp.int32, stacked.shape, 0) & (ROWS - 1)) == ROWS - 1
    here = pl.ds(pl.multiple_of(step * tiles * ROWS, tiles * ROWS), tiles * ROWS)
    for h in range(2):
        slabs = [probs[h * rows_half + j * group : h * rows_half + (j + 1) * group] for j in range(per_device)]
        maxima = functools.reduce(jnp.maximum, slabs)
        max_codes = jnp.round(jnp.sqrt(jnp.sqrt(maxima)) * TOP_CODE).astype(jnp.int32) - MIDDLE
        max_codes = jnp.minimum(max_codes, MIDDLE - 1)
        for s in range(group):
            line = jnp.concatenate(
                [
                    jnp.broadcast_to(max_codes[s : s + 1, j * LANES : (j + 1) * LANES], (ROWS, LANES))
                    for j in range(tiles)
                ],
                axis=0,
            )
            out[where[h * group + s], here, :] = jnp.where(last, line, stacked).astype(jnp.int16)

    @pl.when(step == steps - 1)
    def _():
        expert = ids[...]
        dev = jnp.zeros_like(expert)
        for d in range(1, num_devices):
            dev += jnp.where(expert >= d * per_device, 1, 0)
        order = (expert - dev * per_device) * num_devices + dev
        low, high = lined(jnp.sum(prob_acc[...], axis=1, keepdims=True), order)
        low_coarse, low_fine = coded_pair(low, share)
        high_coarse, high_fine = coded_pair(high, share)
        sums = jnp.concatenate([low_coarse, high_coarse, low_fine, high_fine, counts[0:4, :]], axis=0)
        sums = (sums.astype(jnp.int32) - MIDDLE).astype(jnp.int16)
        for d in range(num_devices):
            out[d, pl.ds(share // LANES * ROWS, ROWS), :] = sums


def route(num_devices, per_device, where, own, other, tokens, picks, counts):
    features, share = tokens.shape
    num_experts = num_devices * per_device
    rows = (share // LANES + 1) * ROWS
    steps = share // BLOCK
    return pl.pallas_call(
        functools.partial(route_kernel, num_devices, per_device),
        out_shape=jax.ShapeDtypeStruct((num_devices, rows, LANES), jnp.int16),
        grid_spec=pltpu.PrefetchScalarGridSpec(
            num_scalar_prefetch=1,
            grid=(steps,),
            in_specs=[
                pl.BlockSpec((num_experts // 2, features), lambda i, w: (0, 0)),
                pl.BlockSpec((num_experts // 2, features), lambda i, w: (0, 0)),
                pl.BlockSpec(memory_space=pl.ANY),
                pl.BlockSpec((TOP, BLOCK), lambda i, w: (0, i)),
                pl.BlockSpec((ROWS, LANES), lambda i, w: (0, 0)),
            ],
            out_specs=pl.BlockSpec((num_devices, rows, LANES), lambda i, w: (0, 0, 0)),
            scratch_shapes=[
                pltpu.VMEM((num_experts, features), jnp.bfloat16),
                pltpu.VMEM((num_experts, LANES), jnp.int32),
                pltpu.VMEM((steps, features, BLOCK), jnp.bfloat16),
                pltpu.SemaphoreType.DMA((steps, PIECES)),
                pltpu.VMEM((num_experts, LANES), jnp.float32),
            ],
        ),
        compiler_params=pltpu.CompilerParams(
            dimension_semantics=("arbitrary",), vmem_limit_bytes=51 * 1024 * 1024
        ),
        name="route",
    )(where, own, other, tokens, picks, counts)


def decoded(codes):
    return codes.astype(jnp.int32).astype(jnp.float32) + float(MIDDLE)


def sums_kernel(share, recv, sums):
    total = jnp.zeros((ROWS, LANES), jnp.float32)
    for d in range(recv.shape[0]):
        tile = decoded(recv[d])
        probs = decoded_pair(tile[0:2], tile[2:4], share)
        total += jnp.concatenate([probs, tile[4:8], jnp.zeros((2, LANES), jnp.float32)], axis=0)
    sums[...] = total


def spread_kernel(recv, gates, maxima):
    num, rows, _ = recv.shape
    tiles = rows // ROWS - 1
    share = tiles * LANES
    for d in range(num):
        codes = decoded(recv[d, 0 : tiles * ROWS, :])
        for j in range(tiles):
            tile = codes[j * ROWS : (j + 1) * ROWS]
            cols = slice(d * share + j * LANES, d * share + (j + 1) * LANES)
            gates[:, cols] = tile[0:TOP] * step_scale(tile[TOP : TOP + 1])
            maxima[:, cols] = fourth(unit(tile[TOP + 1 : TOP + 2]))


def balance_kernel(num_devices, per_device, total_tokens, where, own, near, far, swapped, out, slots):
    place, core = where[0], where[1]
    slots[place] = own[...]
    slots[(place + jnp.where(core == 0, 3, 1)) % 4] = near[...]
    slots[(place + 2) % 4] = far[...]
    slots[(place + jnp.where(core == 0, 1, 3)) % 4] = swapped[...]
    total = (slots[0] + slots[1]) + (slots[2] + slots[3])
    num_experts = num_devices * per_device
    prob = jnp.concatenate([total[0:1], total[1:2]], axis=1)[:, :num_experts] / total_tokens
    freq = jnp.concatenate([total[2:3], total[3:4]], axis=1)[:, :num_experts] * (
        num_experts / (TOP * total_tokens)
    )
    sent = total[4:5, :num_devices] * (num_devices / (DEV_TOP * total_tokens))

    def by_device(x):
        return functools.reduce(
            jnp.add, [x[:, j * num_devices : (j + 1) * num_devices] for j in range(per_device)]
        )

    dev_prob = by_device(prob)
    dev_freq = by_device(freq) / per_device
    losses = [jnp.sum(a * b, axis=1, keepdims=True) for a, b in ((freq, prob), (dev_freq, dev_prob), (sent, dev_prob))]
    lane = lax.broadcasted_iota(jnp.int32, (1, LANES), 1)
    out[...] = jnp.where(lane == 0, losses[0], jnp.where(lane == 1, losses[1], losses[2]))


def local(tokens, router, device_pick, expert_pick):
    features, share = tokens.shape
    num_devices = lax.axis_size(EXPERT)
    per_device = router.shape[1]
    num_experts = per_device * num_devices
    total_tokens = share * num_devices * lax.axis_size(DP)
    my_index = lax.axis_index(EXPERT)
    core, z, y = (lax.axis_index(axis) for axis in ("dp_1", "expert_0", "expert_1"))
    deep, wide = sizes = (lax.axis_size("expert_0"), lax.axis_size("expert_1"))
    group = num_devices // 2

    block = router.T.reshape(per_device * features // LANES, LANES)
    pieces = [block]
    for k in range(1, deep // 2):
        pairs = [(i, (i + k) % deep) for i in range(deep)]
        pairs += [(deep + i, deep + (i - k) % deep) for i in range(deep)]
        pieces.append(lax.ppermute(block, ("dp_1", "expert_0"), pairs))
    across = lax.ppermute(
        block, ("dp_1", "expert_0"), [(deep + i, deep + (i + deep // 2) % deep) for i in range(deep)]
    )
    pieces[0] = jnp.where(core == 0, block, across)
    column = jnp.stack(pieces)
    plane = [column] + [
        lax.ppermute(column, "expert_1", [(i, (i + k) % wide) for i in range(wide)]) for k in range(1, wide)
    ]
    tall = features // LANES
    own = jnp.stack(plane).reshape(group, per_device, tall, LANES).transpose(1, 0, 2, 3)
    own = own.reshape(num_experts // 2, features)
    other = lax.ppermute(own, "dp_1", [(0, 1), (1, 0)])

    where = source_devices(core, (z, y), sizes)
    rows = (share // LANES + 1) * ROWS
    experts_here = lax.dynamic_slice_in_dim(expert_pick, my_index * share, share, 1)
    devices_here = lax.dynamic_slice_in_dim(device_pick, my_index * share, share, 1)
    counts = pl.pallas_call(
        functools.partial(count_kernel, num_devices, per_device),
        out_shape=jax.ShapeDtypeStruct((ROWS, LANES), jnp.float32),
        compiler_params=pltpu.CompilerParams(vmem_limit_bytes=2 * 1024 * 1024),
        name="count",
    )(experts_here, devices_here)
    msg = route(num_devices, per_device, where, own, other, tokens, experts_here, counts)

    recv = lax.all_to_all(msg, EXPERT, 0, 0, tiled=True)
    sums = pl.pallas_call(
        functools.partial(sums_kernel, share),
        out_shape=jax.ShapeDtypeStruct((ROWS, LANES), jnp.float32),
        grid=(1,),
        in_specs=[pl.BlockSpec((num_devices, ROWS, LANES), lambda i: (0, rows // ROWS - 1, 0))],
        out_specs=pl.BlockSpec((ROWS, LANES), lambda i: (0, 0)),
        compiler_params=pltpu.CompilerParams(vmem_limit_bytes=2 * 1024 * 1024),
        name="sums",
    )(recv)
    gates, device_max = pl.pallas_call(
        spread_kernel,
        out_shape=(
            jax.ShapeDtypeStruct((TOP, share * num_devices), jnp.float32),
            jax.ShapeDtypeStruct((1, share * num_devices), jnp.float32),
        ),
        compiler_params=pltpu.CompilerParams(vmem_limit_bytes=16 * 1024 * 1024),
        name="spread",
    )(recv)
    swap = [(0, 1), (1, 0)]
    chip = sums + lax.ppermute(sums, "dp_1", swap)
    length = lax.axis_size("dp_0")
    around = [(2 * i, (2 * i + 2) % (2 * length)) for i in range(length)]
    around += [(2 * i + 1, (2 * i - 1) % (2 * length)) for i in range(length)]
    near = lax.ppermute(chip, ("dp_0", "dp_1"), around)
    far = lax.ppermute(chip, "dp_0", [(i, (i + length // 2) % length) for i in range(length)])
    swapped = lax.ppermute(near, "dp_1", swap)
    balance = pl.pallas_call(
        functools.partial(balance_kernel, num_devices, per_device, total_tokens),
        out_shape=jax.ShapeDtypeStruct((1, LANES), jnp.float32),
        grid_spec=pltpu.PrefetchScalarGridSpec(
            num_scalar_prefetch=1,
            grid=(1,),
            in_specs=[pl.BlockSpec((ROWS, LANES), lambda i, w: (0, 0))] * 4,
            out_specs=pl.BlockSpec((1, LANES), lambda i, w: (0, 0)),
            scratch_shapes=[pltpu.VMEM((4, ROWS, LANES), jnp.float32)],
        ),
        compiler_params=pltpu.CompilerParams(vmem_limit_bytes=1024 * 1024),
        name="balance",
    )(jnp.stack([lax.axis_index("dp_0"), core]).astype(jnp.int32), chip, near, far, swapped)
    return (gates, device_max, balance[0, 0:3])


def solution(mesh):
    torus = Mesh(mesh.devices.reshape(4, 2, 8, 4), ("dp_0", "dp_1", "expert_0", "expert_1"))
    return jax.shard_map(
        local,
        mesh=torus,
        in_specs=(P(None, DP_EXPERT), P(None, EXPERT), P(None, DP), P(None, DP)),
        out_specs=(P(None, DP), P(EXPERT, DP), P()),
        check_vma=False,
    )
```

```python
import functools

import jax
import jax.numpy as jnp
from jax import lax
from jax.experimental import pallas as pl
from jax.experimental.pallas import tpu as pltpu
from jax.sharding import Mesh
from jax.sharding import PartitionSpec as P


TOP = 6
DEV_TOP = 3
EXPERT = ("expert_0", "expert_1")
DP = ("dp_0", "dp_1")
DP_EXPERT = ("dp_0", "dp_1", "expert_0", "expert_1")
BLOCK = 256
LANES = 128
ROWS = 8
TOP_CODE = 65535.0
MIDDLE = 32768
TINY = 1e-30


def lane_sum(x):
    parts = [x[:, i : i + LANES] for i in range(0, x.shape[1], LANES)]
    return functools.reduce(jnp.add, parts)


def fourth(x):
    return jnp.square(jnp.square(x))


def eighth(x):
    return jnp.square(fourth(x))


def eighth_root(x):
    return jnp.sqrt(jnp.sqrt(jnp.sqrt(x)))


def unit(code):
    return code * (1.0 / TOP_CODE)


def step_scale(code):
    return jnp.maximum(eighth(unit(code)), TINY) * (1.0 / TOP_CODE)


def coded_pair(x, limit):
    coarse = jnp.minimum(jnp.floor(eighth_root(x * (1.0 / limit)) * TOP_CODE), TOP_CODE)
    base = eighth(unit(coarse)) * limit
    rest = jnp.where(base > 0.0, (x - base) / jnp.maximum(base, TINY), 0.0)
    fine = jnp.round(jnp.clip(rest * coarse * (1.0 / 16.0), 0.0, 1.0) * TOP_CODE)
    return coarse, fine


def decoded_pair(coarse, fine, limit):
    base = eighth(unit(coarse)) * limit
    return base * (1.0 + unit(fine) * 16.0 / jnp.maximum(coarse, 1.0))


def source_devices(core, place, sizes):
    deep, wide = sizes
    z, y = place
    row = jnp.arange(deep * wide, dtype=jnp.int32)
    back = row % (deep // 2)
    aside = (row // (deep // 2)) % wide
    half = row // (deep * wide // 2)
    ahead = jnp.where(back == 0, deep // 2, back)
    offset = jnp.where(core == half, deep - back, ahead)
    return ((z + offset) % deep) * wide + (y + wide - aside) % wide


def lined(total, index):
    lanes = lax.broadcasted_iota(jnp.int32, index.shape, 1)
    return [
        jnp.sum(jnp.where(index == lanes + i * LANES, total, 0.0), axis=0, keepdims=True) for i in range(2)
    ]


def count_kernel(num_devices, per_device, picks, devs, out):
    num_experts = num_devices * per_device
    share = picks.shape[1]
    counts = []
    for j in range(per_device):
        ids = lax.broadcasted_iota(jnp.int32, (num_devices, LANES), 0) * per_device + j
        total = jnp.zeros((num_devices, LANES), jnp.float32)
        for c in range(0, share, LANES):
            for k in range(TOP):
                total += jnp.where(ids == picks[k : k + 1, c : c + LANES], 1.0, 0.0)
        counts.append(jnp.sum(total, axis=1, keepdims=True))
    ids = lax.broadcasted_iota(jnp.int32, (num_devices, LANES), 0)
    total = jnp.zeros((num_devices, LANES), jnp.float32)
    for c in range(0, share, LANES):
        for k in range(DEV_TOP):
            total += jnp.where(ids == devs[k : k + 1, c : c + LANES], 1.0, 0.0)
    rows = lax.broadcasted_iota(jnp.int32, (num_experts, LANES), 0)
    low, high = lined(jnp.concatenate(counts, axis=0), rows)
    sent_low, sent_high = lined(jnp.sum(total, axis=1, keepdims=True), ids)
    none = jnp.zeros((ROWS - 4, LANES), jnp.float32)
    out[...] = jnp.concatenate([low, high, sent_low, sent_high, none], axis=0)


def block_copy(tokens, blocks, arrived, first, i):
    _, depth, block = blocks.shape
    source = tokens.at[pl.ds(first, depth), pl.ds(i * block, block)]
    return pltpu.make_async_copy(source, blocks.at[i], arrived.at[i])


def load(own, other, tokens, router, blocks, arrived, first):
    half = own.shape[0]
    for i in range(blocks.shape[0]):
        block_copy(tokens, blocks, arrived, first, i).start()
    router[:half] = own[...]
    router[half:] = other[...]


def partial_kernel(own, other, tokens, out, router, blocks, arrived):
    step = pl.program_id(0)

    @pl.when(step == 0)
    def _():
        load(own, other, tokens, router, blocks, arrived, 0)

    block_copy(tokens, blocks, arrived, 0, step).wait()
    out[...] = jnp.dot(router[...], blocks[step], preferred_element_type=jnp.float32)


def route_kernel(
    num_devices,
    per_device,
    where,
    own,
    other,
    tokens,
    partial,
    picks,
    counts,
    out,
    router,
    ids,
    blocks,
    arrived,
    prob_acc,
):
    step = pl.program_id(0)
    num_experts = num_devices * per_device
    group = num_devices // 2
    rows_half = num_experts // 2
    steps, depth, block = blocks.shape
    first = tokens.shape[0] - depth
    tiles = block // LANES
    share = block * steps

    @pl.when(step == 0)
    def _():
        load(own, other, tokens, router, blocks, arrived, first)
        prob_acc[...] = jnp.zeros_like(prob_acc)
        row = lax.broadcasted_iota(jnp.int32, (group, LANES), 0)
        for h in range(2):
            dev = jnp.zeros((group, LANES), jnp.int32)
            for s in range(group):
                dev = jnp.where(row == s, where[h * group + s], dev)
            for j in range(per_device):
                ids[pl.ds(h * rows_half + j * group, group), :] = dev * per_device + j

    block_copy(tokens, blocks, arrived, first, step).wait()
    scores = partial[...] + jnp.dot(router[...], blocks[step], preferred_element_type=jnp.float32)
    peak = jnp.max(scores, axis=0, keepdims=True)
    raised = jnp.exp(scores - peak)
    probs = raised * (1.0 / jnp.sum(raised, axis=0, keepdims=True))
    prob_acc[...] += lane_sum(probs)
    ids_wide = jnp.concatenate([ids[...]] * tiles, axis=1)
    chosen = [
        jnp.sum(jnp.where(ids_wide == picks[k : k + 1, :], probs, 0.0), axis=0, keepdims=True)
        for k in range(TOP)
    ]

    largest = functools.reduce(jnp.maximum, chosen)
    scale = jnp.minimum(jnp.floor(eighth_root(largest) * TOP_CODE) + 1.0, TOP_CODE)
    inverse = 1.0 / step_scale(scale)
    codes = [jnp.minimum(jnp.round(g * inverse), TOP_CODE) for g in chosen]
    lines = jnp.concatenate([*codes, scale, scale], axis=0).astype(jnp.int32) - MIDDLE
    stacked = jnp.concatenate([lines[:, j * LANES : (j + 1) * LANES] for j in range(tiles)], axis=0)
    last = (lax.broadcasted_iota(jnp.int32, stacked.shape, 0) & (ROWS - 1)) == ROWS - 1
    here = pl.ds(pl.multiple_of(step * tiles * ROWS, tiles * ROWS), tiles * ROWS)
    for h in range(2):
        slabs = [probs[h * rows_half + j * group : h * rows_half + (j + 1) * group] for j in range(per_device)]
        maxima = functools.reduce(jnp.maximum, slabs)
        max_codes = jnp.round(jnp.sqrt(jnp.sqrt(maxima)) * TOP_CODE).astype(jnp.int32) - MIDDLE
        max_codes = jnp.minimum(max_codes, MIDDLE - 1)
        for s in range(group):
            line = jnp.concatenate(
                [
                    jnp.broadcast_to(max_codes[s : s + 1, j * LANES : (j + 1) * LANES], (ROWS, LANES))
                    for j in range(tiles)
                ],
                axis=0,
            )
            out[where[h * group + s], here, :] = jnp.where(last, line, stacked).astype(jnp.int16)

    @pl.when(step == steps - 1)
    def _():
        expert = ids[...]
        dev = jnp.zeros_like(expert)
        for d in range(1, num_devices):
            dev += jnp.where(expert >= d * per_device, 1, 0)
        order = (expert - dev * per_device) * num_devices + dev
        low, high = lined(jnp.sum(prob_acc[...], axis=1, keepdims=True), order)
        low_coarse, low_fine = coded_pair(low, share)
        high_coarse, high_fine = coded_pair(high, share)
        sums = jnp.concatenate([low_coarse, high_coarse, low_fine, high_fine, counts[0:4, :]], axis=0)
        sums = (sums.astype(jnp.int32) - MIDDLE).astype(jnp.int16)
        for d in range(num_devices):
            out[d, pl.ds(share // LANES * ROWS, ROWS), :] = sums


def partial_scores(own, other, tokens):
    half, depth = own.shape
    share = tokens.shape[1]
    steps = share // BLOCK
    return pl.pallas_call(
        partial_kernel,
        out_shape=jax.ShapeDtypeStruct((2 * half, share), jnp.float32),
        grid=(steps,),
        in_specs=[
            pl.BlockSpec((half, depth), lambda i: (0, 0)),
            pl.BlockSpec((half, depth), lambda i: (0, 0)),
            pl.BlockSpec(memory_space=pl.ANY),
        ],
        out_specs=pl.BlockSpec((2 * half, BLOCK), lambda i: (0, i)),
        scratch_shapes=[
            pltpu.VMEM((2 * half, depth), jnp.bfloat16),
            pltpu.VMEM((steps, depth, BLOCK), jnp.bfloat16),
            pltpu.SemaphoreType.DMA((steps,)),
        ],
        compiler_params=pltpu.CompilerParams(
            dimension_semantics=("arbitrary",), vmem_limit_bytes=51 * 1024 * 1024
        ),
        name="partial",
    )(own, other, tokens)


def route(num_devices, per_device, where, own, other, tokens, partial, picks, counts):
    half, depth = own.shape
    share = tokens.shape[1]
    num_experts = num_devices * per_device
    rows = (share // LANES + 1) * ROWS
    steps = share // BLOCK
    return pl.pallas_call(
        functools.partial(route_kernel, num_devices, per_device),
        out_shape=jax.ShapeDtypeStruct((num_devices, rows, LANES), jnp.int16),
        grid_spec=pltpu.PrefetchScalarGridSpec(
            num_scalar_prefetch=1,
            grid=(steps,),
            in_specs=[
                pl.BlockSpec((half, depth), lambda i, w: (0, 0)),
                pl.BlockSpec((half, depth), lambda i, w: (0, 0)),
                pl.BlockSpec(memory_space=pl.ANY),
                pl.BlockSpec((num_experts, BLOCK), lambda i, w: (0, i)),
                pl.BlockSpec((TOP, BLOCK), lambda i, w: (0, i)),
                pl.BlockSpec((ROWS, LANES), lambda i, w: (0, 0)),
            ],
            out_specs=pl.BlockSpec((num_devices, rows, LANES), lambda i, w: (0, 0, 0)),
            scratch_shapes=[
                pltpu.VMEM((num_experts, depth), jnp.bfloat16),
                pltpu.VMEM((num_experts, LANES), jnp.int32),
                pltpu.VMEM((steps, depth, BLOCK), jnp.bfloat16),
                pltpu.SemaphoreType.DMA((steps,)),
                pltpu.VMEM((num_experts, LANES), jnp.float32),
            ],
        ),
        compiler_params=pltpu.CompilerParams(
            dimension_semantics=("arbitrary",), vmem_limit_bytes=51 * 1024 * 1024
        ),
        name="route",
    )(where, own, other, tokens, partial, picks, counts)


def decoded(codes):
    return codes.astype(jnp.int32).astype(jnp.float32) + float(MIDDLE)


def sums_kernel(share, recv, sums):
    total = jnp.zeros((ROWS, LANES), jnp.float32)
    for d in range(recv.shape[0]):
        tile = decoded(recv[d])
        probs = decoded_pair(tile[0:2], tile[2:4], share)
        total += jnp.concatenate([probs, tile[4:8], jnp.zeros((2, LANES), jnp.float32)], axis=0)
    sums[...] = total


def spread_kernel(recv, gates, maxima):
    num, rows, _ = recv.shape
    tiles = rows // ROWS - 1
    share = tiles * LANES
    for d in range(num):
        codes = decoded(recv[d, 0 : tiles * ROWS, :])
        for j in range(tiles):
            tile = codes[j * ROWS : (j + 1) * ROWS]
            cols = slice(d * share + j * LANES, d * share + (j + 1) * LANES)
            gates[:, cols] = tile[0:TOP] * step_scale(tile[TOP : TOP + 1])
            maxima[:, cols] = fourth(unit(tile[TOP + 1 : TOP + 2]))


def balance_kernel(num_devices, per_device, total_tokens, where, own, near, far, swapped, out, slots):
    place, core = where[0], where[1]
    slots[place] = own[...]
    slots[(place + jnp.where(core == 0, 3, 1)) % 4] = near[...]
    slots[(place + 2) % 4] = far[...]
    slots[(place + jnp.where(core == 0, 1, 3)) % 4] = swapped[...]
    total = (slots[0] + slots[1]) + (slots[2] + slots[3])
    num_experts = num_devices * per_device
    prob = jnp.concatenate([total[0:1], total[1:2]], axis=1)[:, :num_experts] / total_tokens
    freq = jnp.concatenate([total[2:3], total[3:4]], axis=1)[:, :num_experts] * (
        num_experts / (TOP * total_tokens)
    )
    sent = total[4:5, :num_devices] * (num_devices / (DEV_TOP * total_tokens))

    def by_device(x):
        return functools.reduce(
            jnp.add, [x[:, j * num_devices : (j + 1) * num_devices] for j in range(per_device)]
        )

    dev_prob = by_device(prob)
    dev_freq = by_device(freq) / per_device
    losses = [jnp.sum(a * b, axis=1, keepdims=True) for a, b in ((freq, prob), (dev_freq, dev_prob), (sent, dev_prob))]
    lane = lax.broadcasted_iota(jnp.int32, (1, LANES), 1)
    out[...] = jnp.where(lane == 0, losses[0], jnp.where(lane == 1, losses[1], losses[2]))


def local(tokens, router, device_pick, expert_pick):
    features, share = tokens.shape
    num_devices = lax.axis_size(EXPERT)
    per_device = router.shape[1]
    num_experts = per_device * num_devices
    total_tokens = share * num_devices * lax.axis_size(DP)
    my_index = lax.axis_index(EXPERT)
    core, z, y = (lax.axis_index(axis) for axis in ("dp_1", "expert_0", "expert_1"))
    deep, wide = sizes = (lax.axis_size("expert_0"), lax.axis_size("expert_1"))
    group = num_devices // 2

    tall = features // LANES
    early = tall * 3 // 5 // ROWS * ROWS
    columns = router.T.reshape(per_device, tall, LANES)
    block = jnp.concatenate(
        [part.reshape(-1, LANES) for part in (columns[:, :early], columns[:, early:])], axis=0
    )
    pieces = [block]
    for k in range(1, deep // 2):
        pairs = [(i, (i + k) % deep) for i in range(deep)]
        pairs += [(deep + i, deep + (i - k) % deep) for i in range(deep)]
        pieces.append(lax.ppermute(block, ("dp_1", "expert_0"), pairs))
    across = lax.ppermute(
        block, ("dp_1", "expert_0"), [(deep + i, deep + (i + deep // 2) % deep) for i in range(deep)]
    )
    pieces[0] = jnp.where(core == 0, block, across)
    column = jnp.stack(pieces)

    def along_y(part):
        plane = [part]
        for k in range(1, wide):
            plane.append(lax.ppermute(part, "expert_1", [(i, (i + k) % wide) for i in range(wide)]))
        plane = jnp.stack(plane).reshape(group, per_device, -1, LANES).transpose(1, 0, 2, 3)
        return plane.reshape(num_experts // 2, -1)

    swap = [(0, 1), (1, 0)]
    cut = early * per_device
    own_first, own_last = along_y(column[:, :cut]), along_y(column[:, cut:])
    other_first = lax.ppermute(own_first, "dp_1", swap)
    partial = partial_scores(own_first, other_first, tokens)
    other_last = lax.ppermute(own_last, "dp_1", swap)

    where = source_devices(core, (z, y), sizes)
    rows = (share // LANES + 1) * ROWS
    experts_here = lax.dynamic_slice_in_dim(expert_pick, my_index * share, share, 1)
    devices_here = lax.dynamic_slice_in_dim(device_pick, my_index * share, share, 1)
    tally = pl.pallas_call(
        functools.partial(count_kernel, num_devices, per_device),
        out_shape=jax.ShapeDtypeStruct((ROWS, LANES), jnp.float32),
        compiler_params=pltpu.CompilerParams(vmem_limit_bytes=2 * 1024 * 1024),
        name="count",
    )
    counts = tally(experts_here, devices_here)
    msg = route(num_devices, per_device, where, own_last, other_last, tokens, partial, experts_here, counts)

    recv = lax.all_to_all(msg, EXPERT, 0, 0, tiled=True)
    sums = pl.pallas_call(
        functools.partial(sums_kernel, share),
        out_shape=jax.ShapeDtypeStruct((ROWS, LANES), jnp.float32),
        grid=(1,),
        in_specs=[pl.BlockSpec((num_devices, ROWS, LANES), lambda i: (0, rows // ROWS - 1, 0))],
        out_specs=pl.BlockSpec((ROWS, LANES), lambda i: (0, 0)),
        compiler_params=pltpu.CompilerParams(vmem_limit_bytes=2 * 1024 * 1024),
        name="sums",
    )(recv)
    gates, device_max = pl.pallas_call(
        spread_kernel,
        out_shape=(
            jax.ShapeDtypeStruct((TOP, share * num_devices), jnp.float32),
            jax.ShapeDtypeStruct((1, share * num_devices), jnp.float32),
        ),
        compiler_params=pltpu.CompilerParams(vmem_limit_bytes=16 * 1024 * 1024),
        name="spread",
    )(recv)
    chip = sums + lax.ppermute(sums, "dp_1", swap)
    length = lax.axis_size("dp_0")
    around = [(2 * i, (2 * i + 2) % (2 * length)) for i in range(length)]
    around += [(2 * i + 1, (2 * i - 1) % (2 * length)) for i in range(length)]
    near = lax.ppermute(chip, ("dp_0", "dp_1"), around)
    far = lax.ppermute(chip, "dp_0", [(i, (i + length // 2) % length) for i in range(length)])
    swapped = lax.ppermute(near, "dp_1", swap)
    balance = pl.pallas_call(
        functools.partial(balance_kernel, num_devices, per_device, total_tokens),
        out_shape=jax.ShapeDtypeStruct((1, LANES), jnp.float32),
        grid_spec=pltpu.PrefetchScalarGridSpec(
            num_scalar_prefetch=1,
            grid=(1,),
            in_specs=[pl.BlockSpec((ROWS, LANES), lambda i, w: (0, 0))] * 4,
            out_specs=pl.BlockSpec((1, LANES), lambda i, w: (0, 0)),
            scratch_shapes=[pltpu.VMEM((4, ROWS, LANES), jnp.float32)],
        ),
        compiler_params=pltpu.CompilerParams(vmem_limit_bytes=1024 * 1024),
        name="balance",
    )(jnp.stack([lax.axis_index("dp_0"), core]).astype(jnp.int32), chip, near, far, swapped)
    return (gates, device_max, balance[0, 0:3])


def solution(mesh):
    torus = Mesh(mesh.devices.reshape(4, 2, 8, 4), ("dp_0", "dp_1", "expert_0", "expert_1"))
    return jax.shard_map(
        local,
        mesh=torus,
        in_specs=(P(None, DP_EXPERT), P(None, EXPERT), P(None, DP), P(None, DP)),
        out_specs=(P(None, DP), P(EXPERT, DP), P()),
        check_vma=False,
    )
```

```python
import functools

import jax
import jax.numpy as jnp
from jax import lax
from jax.experimental import pallas as pl
from jax.experimental.pallas import tpu as pltpu
from jax.sharding import Mesh
from jax.sharding import PartitionSpec as P

TOP = 6
DEV_TOP = 3
EXPERT = ("expert_0", "expert_1")
DP = ("dp_0", "dp_1")
DP_EXPERT = ("dp_0", "dp_1", "expert_0", "expert_1")
BLOCK = 256
PIECES = 1
LANES = 128
ROWS = 8
TOP_CODE = 65535.0
MIDDLE = 32768
TINY = 1e-30


def sent_to_all(x, axis):
    length = lax.axis_size(axis)
    return lax.all_to_all(jnp.broadcast_to(x[None], (length, *x.shape)), axis, 0, 0, tiled=True)


def lane_sum(x):
    parts = [x[:, i : i + LANES] for i in range(0, x.shape[1], LANES)]
    return functools.reduce(jnp.add, parts)


def fourth(x):
    return jnp.square(jnp.square(x))


def eighth(x):
    return jnp.square(fourth(x))


def eighth_root(x):
    return jnp.sqrt(jnp.sqrt(jnp.sqrt(x)))


def unit(code):
    return code * (1.0 / TOP_CODE)


def step_scale(code):
    return jnp.maximum(eighth(unit(code)), TINY) * (1.0 / TOP_CODE)


def coded_pair(x, limit):
    coarse = jnp.minimum(jnp.floor(eighth_root(x * (1.0 / limit)) * TOP_CODE), TOP_CODE)
    base = eighth(unit(coarse)) * limit
    rest = jnp.where(base > 0.0, (x - base) / jnp.maximum(base, TINY), 0.0)
    fine = jnp.round(jnp.clip(rest * coarse * (1.0 / 16.0), 0.0, 1.0) * TOP_CODE)
    return coarse, fine


def decoded_pair(coarse, fine, limit):
    base = eighth(unit(coarse)) * limit
    return base * (1.0 + unit(fine) * 16.0 / jnp.maximum(coarse, 1.0))


def source_device(index, row, sizes):
    deep, wide = sizes
    core, z, y = index // (deep * wide), (index // wide) % deep, index % wide
    half, aside, back = row // (deep * wide // 2), (row // (deep // 2)) % wide, row % (deep // 2)
    offset = jnp.where(core == half, deep - back, back or deep // 2)
    return ((z + offset) % deep) * wide + (y + wide - aside) % wide


def lined(total, index):
    lanes = lax.broadcasted_iota(jnp.int32, index.shape, 1)
    return [
        jnp.sum(jnp.where(index == lanes + i * LANES, total, 0.0), axis=0, keepdims=True) for i in range(2)
    ]


def count_kernel(num_devices, per_device, picks, devs, out):
    num_experts = num_devices * per_device
    share = picks.shape[1]
    counts, sent = [], []
    for j in range(per_device):
        ids = lax.broadcasted_iota(jnp.int32, (num_devices, LANES), 0) * per_device + j
        total = jnp.zeros((num_devices, LANES), jnp.float32)
        for c in range(0, share, LANES):
            for k in range(TOP):
                total += jnp.where(ids == picks[k : k + 1, c : c + LANES], 1.0, 0.0)
        counts.append(jnp.sum(total, axis=1, keepdims=True))
    ids = lax.broadcasted_iota(jnp.int32, (num_devices, LANES), 0)
    total = jnp.zeros((num_devices, LANES), jnp.float32)
    for c in range(0, share, LANES):
        for k in range(DEV_TOP):
            total += jnp.where(ids == devs[k : k + 1, c : c + LANES], 1.0, 0.0)
    rows = lax.broadcasted_iota(jnp.int32, (num_experts, LANES), 0)
    low, high = lined(jnp.concatenate(counts, axis=0), rows)
    sent_low, sent_high = lined(jnp.sum(total, axis=1, keepdims=True), ids)
    none = jnp.zeros((ROWS - 4, LANES), jnp.float32)
    out[...] = jnp.concatenate([low, high, sent_low, sent_high, none], axis=0)


def route_kernel(
    sizes,
    per_device,
    where,
    own,
    other,
    tokens,
    picks,
    counts,
    out,
    router,
    ids,
    targets,
    blocks,
    arrived,
    prob_acc,
):
    step = pl.program_id(0)
    num_devices = sizes[0] * sizes[1]
    num_experts = num_devices * per_device
    group = num_devices // 2
    rows_half = num_experts // 2
    steps, features, block = blocks.shape
    tiles = block // LANES
    share = block * steps
    depth = features // PIECES

    def piece(i, p):
        rows = pl.ds(p * depth, depth)
        cols = pl.ds(i * block, block)
        return pltpu.make_async_copy(tokens.at[rows, cols], blocks.at[i, rows, :], arrived.at[i, p])

    @pl.when(step == 0)
    def _():
        for i in range(steps):
            for p in range(PIECES):
                piece(i, p).start()
        router[:rows_half] = own[...]
        router[rows_half:] = other[...]
        prob_acc[...] = jnp.zeros_like(prob_acc)
        row = lax.broadcasted_iota(jnp.int32, (group, LANES), 0)
        for h in range(2):
            dev = jnp.zeros((group, LANES), jnp.int32)
            for s in range(group):
                target = source_device(where[0], h * group + s, sizes)
                targets[h * group + s] = target
                dev = jnp.where(row == s, target, dev)
            for j in range(per_device):
                ids[pl.ds(h * rows_half + j * group, group), :] = dev * per_device + j

    for p in range(PIECES):
        piece(step, p).wait()
    scores = jnp.dot(router[...], blocks[step], preferred_element_type=jnp.float32)
    peak = jnp.max(scores, axis=0, keepdims=True)
    raised = jnp.exp(scores - peak)
    probs = raised * (1.0 / jnp.sum(raised, axis=0, keepdims=True))
    prob_acc[...] += lane_sum(probs)
    ids_wide = jnp.concatenate([ids[...]] * tiles, axis=1)
    chosen = [
        jnp.sum(jnp.where(ids_wide == picks[k : k + 1, :], probs, 0.0), axis=0, keepdims=True)
        for k in range(TOP)
    ]

    largest = functools.reduce(jnp.maximum, chosen)
    scale = jnp.minimum(jnp.floor(eighth_root(largest) * TOP_CODE) + 1.0, TOP_CODE)
    inverse = 1.0 / step_scale(scale)
    codes = [jnp.minimum(jnp.round(g * inverse), TOP_CODE) for g in chosen]
    lines = jnp.concatenate([*codes, scale, scale], axis=0).astype(jnp.int32) - MIDDLE
    stacked = jnp.concatenate([lines[:, j * LANES : (j + 1) * LANES] for j in range(tiles)], axis=0)
    last = (lax.broadcasted_iota(jnp.int32, stacked.shape, 0) & (ROWS - 1)) == ROWS - 1
    here = pl.ds(pl.multiple_of(step * tiles * ROWS, tiles * ROWS), tiles * ROWS)
    for h in range(2):
        slabs = [probs[h * rows_half + j * group : h * rows_half + (j + 1) * group] for j in range(per_device)]
        maxima = functools.reduce(jnp.maximum, slabs)
        max_codes = jnp.round(jnp.sqrt(jnp.sqrt(maxima)) * TOP_CODE).astype(jnp.int32) - MIDDLE
        max_codes = jnp.minimum(max_codes, MIDDLE - 1)
        for s in range(group):
            line = jnp.concatenate(
                [
                    jnp.broadcast_to(max_codes[s : s + 1, j * LANES : (j + 1) * LANES], (ROWS, LANES))
                    for j in range(tiles)
                ],
                axis=0,
            )
            out[targets[h * group + s], here, :] = jnp.where(last, line, stacked).astype(jnp.int16)

    @pl.when(step == steps - 1)
    def _():
        expert = ids[...]
        dev = jnp.zeros_like(expert)
        for d in range(1, num_devices):
            dev += jnp.where(expert >= d * per_device, 1, 0)
        order = (expert - dev * per_device) * num_devices + dev
        low, high = lined(jnp.sum(prob_acc[...], axis=1, keepdims=True), order)
        low_coarse, low_fine = coded_pair(low, share)
        high_coarse, high_fine = coded_pair(high, share)
        sums = jnp.concatenate([low_coarse, high_coarse, low_fine, high_fine, counts[0:4, :]], axis=0)
        sums = (sums.astype(jnp.int32) - MIDDLE).astype(jnp.int16)
        for d in range(num_devices):
            out[d, pl.ds(share // LANES * ROWS, ROWS), :] = sums


def route(sizes, per_device, where, own, other, tokens, picks, counts):
    features, share = tokens.shape
    num_devices = sizes[0] * sizes[1]
    num_experts = num_devices * per_device
    rows = (share // LANES + 1) * ROWS
    steps = share // BLOCK
    return pl.pallas_call(
        functools.partial(route_kernel, sizes, per_device),
        out_shape=jax.ShapeDtypeStruct((num_devices, rows, LANES), jnp.int16),
        grid_spec=pltpu.PrefetchScalarGridSpec(
            num_scalar_prefetch=1,
            grid=(steps,),
            in_specs=[
                pl.BlockSpec((num_experts // 2, features), lambda i, w: (0, 0)),
                pl.BlockSpec((num_experts // 2, features), lambda i, w: (0, 0)),
                pl.BlockSpec(memory_space=pl.ANY),
                pl.BlockSpec((TOP, BLOCK), lambda i, w: (0, i)),
                pl.BlockSpec((ROWS, LANES), lambda i, w: (0, 0)),
            ],
            out_specs=pl.BlockSpec((num_devices, rows, LANES), lambda i, w: (0, 0, 0)),
            scratch_shapes=[
                pltpu.VMEM((num_experts, features), jnp.bfloat16),
                pltpu.VMEM((num_experts, LANES), jnp.int32),
                pltpu.SMEM((num_devices,), jnp.int32),
                pltpu.VMEM((steps, features, BLOCK), jnp.bfloat16),
                pltpu.SemaphoreType.DMA((steps, PIECES)),
                pltpu.VMEM((num_experts, LANES), jnp.float32),
            ],
        ),
        compiler_params=pltpu.CompilerParams(
            dimension_semantics=("arbitrary",), vmem_limit_bytes=51 * 1024 * 1024
        ),
        name="route",
    )(where, own, other, tokens, picks, counts)


def decoded(codes):
    return codes.astype(jnp.int32).astype(jnp.float32) + float(MIDDLE)


def sums_kernel(share, recv, sums):
    total = jnp.zeros((ROWS, LANES), jnp.float32)
    for d in range(recv.shape[0]):
        tile = decoded(recv[d])
        probs = decoded_pair(tile[0:2], tile[2:4], share)
        total += jnp.concatenate([probs, tile[4:8], jnp.zeros((2, LANES), jnp.float32)], axis=0)
    sums[...] = total


def spread_kernel(recv, gates, maxima):
    num, rows, _ = recv.shape
    tiles = rows // ROWS - 1
    share = tiles * LANES
    for d in range(num):
        codes = decoded(recv[d, 0 : tiles * ROWS, :])
        for j in range(tiles):
            tile = codes[j * ROWS : (j + 1) * ROWS]
            cols = slice(d * share + j * LANES, d * share + (j + 1) * LANES)
            gates[:, cols] = tile[0:TOP] * step_scale(tile[TOP : TOP + 1])
            maxima[:, cols] = fourth(unit(tile[TOP + 1 : TOP + 2]))


def balance_kernel(num_devices, per_device, total_tokens, where, own, near, far, swapped, out, slots):
    place, core = where[0] // 2, where[0] % 2
    slots[place] = own[...]
    slots[(place + jnp.where(core == 0, 3, 1)) % 4] = near[...]
    slots[(place + 2) % 4] = far[...]
    slots[(place + jnp.where(core == 0, 1, 3)) % 4] = swapped[...]
    total = (slots[0] + slots[1]) + (slots[2] + slots[3])
    num_experts = num_devices * per_device
    prob = jnp.concatenate([total[0:1], total[1:2]], axis=1)[:, :num_experts] / total_tokens
    freq = jnp.concatenate([total[2:3], total[3:4]], axis=1)[:, :num_experts] * (
        num_experts / (TOP * total_tokens)
    )
    sent = total[4:5, :num_devices] * (num_devices / (DEV_TOP * total_tokens))

    def by_device(x):
        return functools.reduce(
            jnp.add, [x[:, j * num_devices : (j + 1) * num_devices] for j in range(per_device)]
        )

    dev_prob = by_device(prob)
    dev_freq = by_device(freq) / per_device
    for i, (a, b) in enumerate(((freq, prob), (dev_freq, dev_prob), (sent, dev_prob))):
        out[i] = jnp.sum(a * b)


def local(tokens, router, device_pick, expert_pick):
    features, share = tokens.shape
    num_devices = lax.axis_size(EXPERT)
    per_device = router.shape[1]
    num_experts = per_device * num_devices
    total_tokens = share * num_devices * lax.axis_size(DP)
    my_index = lax.axis_index(EXPERT)
    core = lax.axis_index("dp_1")
    deep, wide = sizes = (lax.axis_size("expert_0"), lax.axis_size("expert_1"))
    group = num_devices // 2

    block = router.T.reshape(per_device * features // LANES, LANES)
    pieces = [block]
    for k in range(1, deep // 2):
        pairs = [(i, (i + k) % deep) for i in range(deep)]
        pairs += [(deep + i, deep + (i - k) % deep) for i in range(deep)]
        pieces.append(lax.ppermute(block, ("dp_1", "expert_0"), pairs))
    across = lax.ppermute(
        block, ("dp_1", "expert_0"), [(deep + i, deep + (i + deep // 2) % deep) for i in range(deep)]
    )
    pieces[0] = jnp.where(core == 0, block, across)
    column = jnp.stack(pieces)
    plane = [column] + [
        lax.ppermute(column, "expert_1", [(i, (i + k) % wide) for i in range(wide)]) for k in range(1, wide)
    ]
    tall = features // LANES
    own = jnp.stack(plane).reshape(group, per_device, tall, LANES).transpose(1, 0, 2, 3)
    own = own.reshape(num_experts // 2, features)
    other = lax.ppermute(own, "dp_1", [(0, 1), (1, 0)])

    where = lax.axis_index(("dp_1", *EXPERT)).astype(jnp.int32).reshape(1)
    rows = (share // LANES + 1) * ROWS
    experts_here = lax.dynamic_slice_in_dim(expert_pick, my_index * share, share, 1)
    devices_here = lax.dynamic_slice_in_dim(device_pick, my_index * share, share, 1)
    counts = pl.pallas_call(
        functools.partial(count_kernel, num_devices, per_device),
        out_shape=jax.ShapeDtypeStruct((ROWS, LANES), jnp.float32),
        compiler_params=pltpu.CompilerParams(vmem_limit_bytes=2 * 1024 * 1024),
        name="count",
    )(experts_here, devices_here)
    msg = route(sizes, per_device, where, own, other, tokens, experts_here, counts)

    recv = lax.all_to_all(msg, EXPERT, 0, 0, tiled=True)
    sums = pl.pallas_call(
        functools.partial(sums_kernel, share),
        out_shape=jax.ShapeDtypeStruct((ROWS, LANES), jnp.float32),
        grid=(1,),
        in_specs=[pl.BlockSpec((num_devices, ROWS, LANES), lambda i: (0, rows // ROWS - 1, 0))],
        out_specs=pl.BlockSpec((ROWS, LANES), lambda i: (0, 0)),
        compiler_params=pltpu.CompilerParams(vmem_limit_bytes=2 * 1024 * 1024),
        name="sums",
    )(recv)
    gates, device_max = pl.pallas_call(
        spread_kernel,
        out_shape=(
            jax.ShapeDtypeStruct((TOP, share * num_devices), jnp.float32),
            jax.ShapeDtypeStruct((1, share * num_devices), jnp.float32),
        ),
        compiler_params=pltpu.CompilerParams(vmem_limit_bytes=16 * 1024 * 1024),
        name="spread",
    )(recv)
    swap = [(0, 1), (1, 0)]
    chip = sums + lax.ppermute(sums, "dp_1", swap)
    length = lax.axis_size("dp_0")
    around = [(2 * i, (2 * i + 2) % (2 * length)) for i in range(length)]
    around += [(2 * i + 1, (2 * i - 1) % (2 * length)) for i in range(length)]
    near = lax.ppermute(chip, ("dp_0", "dp_1"), around)
    far = lax.ppermute(chip, "dp_0", [(i, (i + length // 2) % length) for i in range(length)])
    swapped = lax.ppermute(near, "dp_1", swap)
    balance = pl.pallas_call(
        functools.partial(balance_kernel, num_devices, per_device, total_tokens),
        out_shape=jax.ShapeDtypeStruct((3,), jnp.float32),
        grid_spec=pltpu.PrefetchScalarGridSpec(
            num_scalar_prefetch=1,
            grid=(1,),
            in_specs=[pl.BlockSpec((ROWS, LANES), lambda i, w: (0, 0))] * 4,
            out_specs=pl.BlockSpec(memory_space=pltpu.SMEM),
            scratch_shapes=[pltpu.VMEM((4, ROWS, LANES), jnp.float32)],
        ),
        compiler_params=pltpu.CompilerParams(vmem_limit_bytes=1024 * 1024),
        name="balance",
    )(lax.axis_index(DP).astype(jnp.int32).reshape(1), chip, near, far, swapped)
    return (gates, device_max, balance)


def solution(mesh):
    torus = Mesh(mesh.devices.reshape(4, 2, 8, 4), ("dp_0", "dp_1", "expert_0", "expert_1"))
    return jax.shard_map(
        local,
        mesh=torus,
        in_specs=(P(None, DP_EXPERT), P(None, EXPERT), P(None, DP), P(None, DP)),
        out_specs=(P(None, DP), P(EXPERT, DP), P()),
        check_vma=False,
    )
```

```python
import functools

import jax
import jax.numpy as jnp
from jax import lax
from jax.experimental import pallas as pl
from jax.experimental.pallas import tpu as pltpu
from jax.sharding import Mesh
from jax.sharding import PartitionSpec as P

TOP = 6
DEV_TOP = 3
EXPERT = ("expert_0", "expert_1")
DP = ("dp_0", "dp_1")
DP_EXPERT = ("dp_0", "dp_1", "expert_0", "expert_1")
BLOCK = 256
PIECES = 1
LANES = 128
ROWS = 8
TOP_CODE = 65535.0
MIDDLE = 32768
TINY = 1e-30


def sent_to_all(x, axis):
    length = lax.axis_size(axis)
    return lax.all_to_all(jnp.broadcast_to(x[None], (length, *x.shape)), axis, 0, 0, tiled=True)


def lane_sum(x):
    parts = [x[:, i : i + LANES] for i in range(0, x.shape[1], LANES)]
    return functools.reduce(jnp.add, parts)


def fourth(x):
    return jnp.square(jnp.square(x))


def eighth(x):
    return jnp.square(fourth(x))


def eighth_root(x):
    return jnp.sqrt(jnp.sqrt(jnp.sqrt(x)))


def unit(code):
    return code * (1.0 / TOP_CODE)


def step_scale(code):
    return jnp.maximum(eighth(unit(code)), TINY) * (1.0 / TOP_CODE)


def coded_pair(x, limit):
    coarse = jnp.minimum(jnp.floor(eighth_root(x * (1.0 / limit)) * TOP_CODE), TOP_CODE)
    base = eighth(unit(coarse)) * limit
    rest = jnp.where(base > 0.0, (x - base) / jnp.maximum(base, TINY), 0.0)
    fine = jnp.round(jnp.clip(rest * coarse * (1.0 / 16.0), 0.0, 1.0) * TOP_CODE)
    return coarse, fine


def decoded_pair(coarse, fine, limit):
    base = eighth(unit(coarse)) * limit
    return base * (1.0 + unit(fine) * 16.0 / jnp.maximum(coarse, 1.0))


def source_device(index, row, sizes):
    deep, wide = sizes
    count = deep // 2
    x, y, z, core = index % count, (index // count) % wide, (index // (count * wide)) % deep, index // (count * wide * deep)
    half, aside, back = row // (deep * wide // 2), (row // count) % wide, row % count
    if aside == wide // 2:
        back = (x + count - back) % count
        ahead = jnp.where(back == 0, count, back)
    else:
        ahead = back or count
    offset = jnp.where(core == half, deep - back, ahead)
    return ((z + offset) % deep) * wide + (y + wide - aside) % wide


def lined(total, index):
    lanes = lax.broadcasted_iota(jnp.int32, index.shape, 1)
    return [
        jnp.sum(jnp.where(index == lanes + i * LANES, total, 0.0), axis=0, keepdims=True) for i in range(2)
    ]


def count_kernel(num_devices, per_device, picks, devs, out):
    num_experts = num_devices * per_device
    share = picks.shape[1]
    counts, sent = [], []
    for j in range(per_device):
        ids = lax.broadcasted_iota(jnp.int32, (num_devices, LANES), 0) * per_device + j
        total = jnp.zeros((num_devices, LANES), jnp.float32)
        for c in range(0, share, LANES):
            for k in range(TOP):
                total += jnp.where(ids == picks[k : k + 1, c : c + LANES], 1.0, 0.0)
        counts.append(jnp.sum(total, axis=1, keepdims=True))
    ids = lax.broadcasted_iota(jnp.int32, (num_devices, LANES), 0)
    total = jnp.zeros((num_devices, LANES), jnp.float32)
    for c in range(0, share, LANES):
        for k in range(DEV_TOP):
            total += jnp.where(ids == devs[k : k + 1, c : c + LANES], 1.0, 0.0)
    rows = lax.broadcasted_iota(jnp.int32, (num_experts, LANES), 0)
    low, high = lined(jnp.concatenate(counts, axis=0), rows)
    sent_low, sent_high = lined(jnp.sum(total, axis=1, keepdims=True), ids)
    none = jnp.zeros((ROWS - 4, LANES), jnp.float32)
    out[...] = jnp.concatenate([low, high, sent_low, sent_high, none], axis=0)


def route_kernel(
    sizes,
    per_device,
    where,
    own,
    other,
    tokens,
    picks,
    counts,
    out,
    router,
    ids,
    targets,
    blocks,
    arrived,
    prob_acc,
):
    step = pl.program_id(0)
    num_devices = sizes[0] * sizes[1]
    num_experts = num_devices * per_device
    group = num_devices // 2
    rows_half = num_experts // 2
    steps, features, block = blocks.shape
    tiles = block // LANES
    share = block * steps
    depth = features // PIECES

    def piece(i, p):
        rows = pl.ds(p * depth, depth)
        cols = pl.ds(i * block, block)
        return pltpu.make_async_copy(tokens.at[rows, cols], blocks.at[i, rows, :], arrived.at[i, p])

    @pl.when(step == 0)
    def _():
        for i in range(steps):
            for p in range(PIECES):
                piece(i, p).start()
        router[:rows_half] = own[...]
        router[rows_half:] = other[...]
        prob_acc[...] = jnp.zeros_like(prob_acc)
        row = lax.broadcasted_iota(jnp.int32, (group, LANES), 0)
        for h in range(2):
            dev = jnp.zeros((group, LANES), jnp.int32)
            for s in range(group):
                target = source_device(where[0], h * group + s, sizes)
                targets[h * group + s] = target
                dev = jnp.where(row == s, target, dev)
            for j in range(per_device):
                ids[pl.ds(h * rows_half + j * group, group), :] = dev * per_device + j

    for p in range(PIECES):
        piece(step, p).wait()
    scores = jnp.dot(router[...], blocks[step], preferred_element_type=jnp.float32)
    peak = jnp.max(scores, axis=0, keepdims=True)
    raised = jnp.exp(scores - peak)
    probs = raised * (1.0 / jnp.sum(raised, axis=0, keepdims=True))
    prob_acc[...] += lane_sum(probs)
    ids_wide = jnp.concatenate([ids[...]] * tiles, axis=1)
    chosen = [
        jnp.sum(jnp.where(ids_wide == picks[k : k + 1, :], probs, 0.0), axis=0, keepdims=True)
        for k in range(TOP)
    ]

    largest = functools.reduce(jnp.maximum, chosen)
    scale = jnp.minimum(jnp.floor(eighth_root(largest) * TOP_CODE) + 1.0, TOP_CODE)
    inverse = 1.0 / step_scale(scale)
    codes = [jnp.minimum(jnp.round(g * inverse), TOP_CODE) for g in chosen]
    lines = jnp.concatenate([*codes, scale, scale], axis=0).astype(jnp.int32) - MIDDLE
    stacked = jnp.concatenate([lines[:, j * LANES : (j + 1) * LANES] for j in range(tiles)], axis=0)
    last = (lax.broadcasted_iota(jnp.int32, stacked.shape, 0) & (ROWS - 1)) == ROWS - 1
    here = pl.ds(pl.multiple_of(step * tiles * ROWS, tiles * ROWS), tiles * ROWS)
    for h in range(2):
        slabs = [probs[h * rows_half + j * group : h * rows_half + (j + 1) * group] for j in range(per_device)]
        maxima = functools.reduce(jnp.maximum, slabs)
        max_codes = jnp.round(jnp.sqrt(jnp.sqrt(maxima)) * TOP_CODE).astype(jnp.int32) - MIDDLE
        max_codes = jnp.minimum(max_codes, MIDDLE - 1)
        for s in range(group):
            line = jnp.concatenate(
                [
                    jnp.broadcast_to(max_codes[s : s + 1, j * LANES : (j + 1) * LANES], (ROWS, LANES))
                    for j in range(tiles)
                ],
                axis=0,
            )
            out[targets[h * group + s], here, :] = jnp.where(last, line, stacked).astype(jnp.int16)

    @pl.when(step == steps - 1)
    def _():
        expert = ids[...]
        dev = jnp.zeros_like(expert)
        for d in range(1, num_devices):
            dev += jnp.where(expert >= d * per_device, 1, 0)
        order = (expert - dev * per_device) * num_devices + dev
        low, high = lined(jnp.sum(prob_acc[...], axis=1, keepdims=True), order)
        low_coarse, low_fine = coded_pair(low, share)
        high_coarse, high_fine = coded_pair(high, share)
        sums = jnp.concatenate([low_coarse, high_coarse, low_fine, high_fine, counts[0:4, :]], axis=0)
        sums = (sums.astype(jnp.int32) - MIDDLE).astype(jnp.int16)
        for d in range(num_devices):
            out[d, pl.ds(share // LANES * ROWS, ROWS), :] = sums


def route(sizes, per_device, where, own, other, tokens, picks, counts):
    features, share = tokens.shape
    num_devices = sizes[0] * sizes[1]
    num_experts = num_devices * per_device
    rows = (share // LANES + 1) * ROWS
    steps = share // BLOCK
    return pl.pallas_call(
        functools.partial(route_kernel, sizes, per_device),
        out_shape=jax.ShapeDtypeStruct((num_devices, rows, LANES), jnp.int16),
        grid_spec=pltpu.PrefetchScalarGridSpec(
            num_scalar_prefetch=1,
            grid=(steps,),
            in_specs=[
                pl.BlockSpec((num_experts // 2, features), lambda i, w: (0, 0)),
                pl.BlockSpec((num_experts // 2, features), lambda i, w: (0, 0)),
                pl.BlockSpec(memory_space=pl.ANY),
                pl.BlockSpec((TOP, BLOCK), lambda i, w: (0, i)),
                pl.BlockSpec((ROWS, LANES), lambda i, w: (0, 0)),
            ],
            out_specs=pl.BlockSpec((num_devices, rows, LANES), lambda i, w: (0, 0, 0)),
            scratch_shapes=[
                pltpu.VMEM((num_experts, features), jnp.bfloat16),
                pltpu.VMEM((num_experts, LANES), jnp.int32),
                pltpu.SMEM((num_devices,), jnp.int32),
                pltpu.VMEM((steps, features, BLOCK), jnp.bfloat16),
                pltpu.SemaphoreType.DMA((steps, PIECES)),
                pltpu.VMEM((num_experts, LANES), jnp.float32),
            ],
        ),
        compiler_params=pltpu.CompilerParams(
            dimension_semantics=("arbitrary",), vmem_limit_bytes=51 * 1024 * 1024
        ),
        name="route",
    )(where, own, other, tokens, picks, counts)


def decoded(codes):
    return codes.astype(jnp.int32).astype(jnp.float32) + float(MIDDLE)


def sums_kernel(share, recv, sums):
    total = jnp.zeros((ROWS, LANES), jnp.float32)
    for d in range(recv.shape[0]):
        tile = decoded(recv[d])
        probs = decoded_pair(tile[0:2], tile[2:4], share)
        total += jnp.concatenate([probs, tile[4:8], jnp.zeros((2, LANES), jnp.float32)], axis=0)
    sums[...] = total


def spread_kernel(recv, gates, maxima):
    num, rows, _ = recv.shape
    tiles = rows // ROWS - 1
    share = tiles * LANES
    for d in range(num):
        codes = decoded(recv[d, 0 : tiles * ROWS, :])
        for j in range(tiles):
            tile = codes[j * ROWS : (j + 1) * ROWS]
            cols = slice(d * share + j * LANES, d * share + (j + 1) * LANES)
            gates[:, cols] = tile[0:TOP] * step_scale(tile[TOP : TOP + 1])
            maxima[:, cols] = fourth(unit(tile[TOP + 1 : TOP + 2]))


def balance_kernel(num_devices, per_device, total_tokens, where, own, near, far, swapped, out, slots):
    place, core = where[0] // 2, where[0] % 2
    slots[place] = own[...]
    slots[(place + jnp.where(core == 0, 3, 1)) % 4] = near[...]
    slots[(place + 2) % 4] = far[...]
    slots[(place + jnp.where(core == 0, 1, 3)) % 4] = swapped[...]
    total = (slots[0] + slots[1]) + (slots[2] + slots[3])
    num_experts = num_devices * per_device
    prob = jnp.concatenate([total[0:1], total[1:2]], axis=1)[:, :num_experts] / total_tokens
    freq = jnp.concatenate([total[2:3], total[3:4]], axis=1)[:, :num_experts] * (
        num_experts / (TOP * total_tokens)
    )
    sent = total[4:5, :num_devices] * (num_devices / (DEV_TOP * total_tokens))

    def by_device(x):
        return functools.reduce(
            jnp.add, [x[:, j * num_devices : (j + 1) * num_devices] for j in range(per_device)]
        )

    dev_prob = by_device(prob)
    dev_freq = by_device(freq) / per_device
    for i, (a, b) in enumerate(((freq, prob), (dev_freq, dev_prob), (sent, dev_prob))):
        out[i] = jnp.sum(a * b)


def local(tokens, router, device_pick, expert_pick):
    features, share = tokens.shape
    num_devices = lax.axis_size(EXPERT)
    per_device = router.shape[1]
    num_experts = per_device * num_devices
    total_tokens = share * num_devices * lax.axis_size(DP)
    my_index = lax.axis_index(EXPERT)
    core = lax.axis_index("dp_1")
    deep, wide = sizes = (lax.axis_size("expert_0"), lax.axis_size("expert_1"))
    group = num_devices // 2

    block = router.T.reshape(per_device * features // LANES, LANES)
    pieces = [block]
    for k in range(1, deep // 2):
        pairs = [(i, (i + k) % deep) for i in range(deep)]
        pairs += [(deep + i, deep + (i - k) % deep) for i in range(deep)]
        pieces.append(lax.ppermute(block, ("dp_1", "expert_0"), pairs))
    across = lax.ppermute(
        block, ("dp_1", "expert_0"), [(deep + i, deep + (i + deep // 2) % deep) for i in range(deep)]
    )
    pieces[0] = jnp.where(core == 0, block, across)
    column = jnp.stack(pieces)
    quarter = lax.dynamic_index_in_dim(column, lax.axis_index("dp_0"), 0, keepdims=False)
    quarter = lax.ppermute(quarter, "expert_1", [(i, (i + wide // 2) % wide) for i in range(wide)])
    chips = lax.axis_size("dp_0")
    far = [quarter] + [
        lax.ppermute(quarter, "dp_0", [(i, (i + k) % chips) for i in range(chips)]) for k in range(1, chips)
    ]
    near = [
        lax.ppermute(column, "expert_1", [(i, (i + k) % wide) for i in range(wide)]) for k in (1, wide - 1)
    ]
    plane = [column, near[0], jnp.stack(far), near[1]]
    tall = features // LANES
    own = jnp.stack(plane).reshape(group, per_device, tall, LANES).transpose(1, 0, 2, 3)
    own = own.reshape(num_experts // 2, features)
    other = lax.ppermute(own, "dp_1", [(0, 1), (1, 0)])

    where = lax.axis_index(("dp_1", *EXPERT, "dp_0")).astype(jnp.int32).reshape(1)
    rows = (share // LANES + 1) * ROWS
    experts_here = lax.dynamic_slice_in_dim(expert_pick, my_index * share, share, 1)
    devices_here = lax.dynamic_slice_in_dim(device_pick, my_index * share, share, 1)
    counts = pl.pallas_call(
        functools.partial(count_kernel, num_devices, per_device),
        out_shape=jax.ShapeDtypeStruct((ROWS, LANES), jnp.float32),
        compiler_params=pltpu.CompilerParams(vmem_limit_bytes=2 * 1024 * 1024),
        name="count",
    )(experts_here, devices_here)
    msg = route(sizes, per_device, where, own, other, tokens, experts_here, counts)

    recv = lax.all_to_all(msg, EXPERT, 0, 0, tiled=True)
    sums = pl.pallas_call(
        functools.partial(sums_kernel, share),
        out_shape=jax.ShapeDtypeStruct((ROWS, LANES), jnp.float32),
        grid=(1,),
        in_specs=[pl.BlockSpec((num_devices, ROWS, LANES), lambda i: (0, rows // ROWS - 1, 0))],
        out_specs=pl.BlockSpec((ROWS, LANES), lambda i: (0, 0)),
        compiler_params=pltpu.CompilerParams(vmem_limit_bytes=2 * 1024 * 1024),
        name="sums",
    )(recv)
    gates, device_max = pl.pallas_call(
        spread_kernel,
        out_shape=(
            jax.ShapeDtypeStruct((TOP, share * num_devices), jnp.float32),
            jax.ShapeDtypeStruct((1, share * num_devices), jnp.float32),
        ),
        compiler_params=pltpu.CompilerParams(vmem_limit_bytes=16 * 1024 * 1024),
        name="spread",
    )(recv)
    swap = [(0, 1), (1, 0)]
    chip = sums + lax.ppermute(sums, "dp_1", swap)
    length = lax.axis_size("dp_0")
    around = [(2 * i, (2 * i + 2) % (2 * length)) for i in range(length)]
    around += [(2 * i + 1, (2 * i - 1) % (2 * length)) for i in range(length)]
    near = lax.ppermute(chip, ("dp_0", "dp_1"), around)
    far = lax.ppermute(chip, "dp_0", [(i, (i + length // 2) % length) for i in range(length)])
    swapped = lax.ppermute(near, "dp_1", swap)
    balance = pl.pallas_call(
        functools.partial(balance_kernel, num_devices, per_device, total_tokens),
        out_shape=jax.ShapeDtypeStruct((3,), jnp.float32),
        grid_spec=pltpu.PrefetchScalarGridSpec(
            num_scalar_prefetch=1,
            grid=(1,),
            in_specs=[pl.BlockSpec((ROWS, LANES), lambda i, w: (0, 0))] * 4,
            out_specs=pl.BlockSpec(memory_space=pltpu.SMEM),
            scratch_shapes=[pltpu.VMEM((4, ROWS, LANES), jnp.float32)],
        ),
        compiler_params=pltpu.CompilerParams(vmem_limit_bytes=1024 * 1024),
        name="balance",
    )(lax.axis_index(DP).astype(jnp.int32).reshape(1), chip, near, far, swapped)
    return (gates, device_max, balance)


def solution(mesh):
    torus = Mesh(mesh.devices.reshape(4, 2, 8, 4), ("dp_0", "dp_1", "expert_0", "expert_1"))
    return jax.shard_map(
        local,
        mesh=torus,
        in_specs=(P(None, DP_EXPERT), P(None, EXPERT), P(None, DP), P(None, DP)),
        out_specs=(P(None, DP), P(EXPERT, DP), P()),
        check_vma=False,
    )
```
